32 devices in a mesh: gy: 8 (over z, x), gx: 4 (over y, core).
Axes of the slice: x: 2, y: 2, z: 4, core: 2. Of those that a mesh axis runs over, the one named last changes fastest.
Arguments:
- imbalance: float32 [4, 1024, 2048], P(None, 'gy', 'gx'), may hold values from -9 to 9
- flow: float32 [2, 4, 1024, 2048], P(None, None, 'gy', 'gx'), may hold values from -3 to 3
- potential: float32 [4, 1024, 2048], P(None, 'gy', 'gx'), may hold values from -5 to 5
- cost: float32 [1024, 2048], P('gy', 'gx'), may hold values from 0.2 to 2
Outputs:
- flow_out: float32 [2, 4, 1024, 2048], P(None, None, 'gy', 'gx')
- potential_out: float32 [4, 1024, 2048], P(None, 'gy', 'gx')
- residual: float32 [4], replicated
The draws below stay inside these ranges and needn't reach their ends.
All inputs are finite; a program needn't handle non-finite values.
Results may differ from the reference program's by a relative error of at most 0.0001.
Values sent between devices are 32-bit elements; how exact they have to be, the bound alone decides.
A program may use at most 64 MiB of HBM per device.

```python
import math
from functools import partial
import jax
import jax.numpy as jnp
from jax import lax

PAIRS = 4
ITERS = 12
NR = 1024
NC = 2048


def draw_imbalance(key, part):
    row_pos = jnp.arange(NR, dtype=jnp.float32) / max(NR - 1, 1)
    col_pos = jnp.arange(NC, dtype=jnp.float32) / max(NC - 1, 1)
    envelope = 0.25 * (1.0 + 2.0 * row_pos)[:, None] * (1.0 + 2.0 * col_pos)[None, :]
    values = envelope * jnp.clip(jax.random.normal(key, (PAIRS, NR, NC), jnp.float32), -3.5, 3.5)
    return jnp.clip(values, -9.0, 9.0)


def shard_levels(rng, extent, cuts, low, largest):
    loudness = 1.0
    for dim, shards_of in cuts:
        draws = jax.random.uniform(jax.random.fold_in(jax.random.fold_in(rng, 6), dim), (shards_of,), jnp.float32, low / len(cuts), largest / len(cuts))
        loudness = loudness * jnp.repeat(jnp.exp(draws), extent[dim] // shards_of).reshape((-1,) + (1,) * (len(extent) - 1 - dim))
    return loudness


def centred(own_key, dims, spread, bound, pieces=(), held_as=jnp.bfloat16):
    array = jax.random.normal(own_key, dims, jnp.float32) * spread
    if len(pieces) > 0:
        array = shard_levels(own_key, dims, pieces, -0.22, 0.18) * array
    return jnp.clip(array, min=-bound, max=bound).astype(held_as)


def setup_inputs(seed: int = 0) -> dict:
    arg_keys = jax.random.split(jax.random.key(seed), 5)
    imbalance = draw_imbalance(jax.random.fold_in(arg_keys[4], 71), 0)
    flow = centred(arg_keys[1], (2, PAIRS, NR, NC), 0.5, 3.0, ((2, 8), (3, 4)), jnp.float32)
    potential = centred(arg_keys[2], (PAIRS, NR, NC), 1.0, 5.0, ((1, 8), (2, 4)), jnp.float32)
    cost = jnp.clip(jnp.exp(math.log(2.0) - 2.3025851 * jax.random.uniform(arg_keys[3], (NR, NC), jnp.float32) ** shard_levels(arg_keys[3], (NR, NC), ((0, 8), (1, 4)), -0.2, 0.2)), 0.2, 2.0)
    return {"imbalance": imbalance, "flow": flow, "potential": potential, "cost": cost}


initial_step = 0.35
epsilon = 1e-06

def gradient(potential):
    from_below = jnp.concatenate([potential[1:], jnp.zeros_like(potential[:1])], 0)
    from_right = jnp.concatenate([potential[:, 1:], jnp.zeros_like(potential[:, :1])], 1)
    return (from_below - potential, from_right - potential)

def divergence(flow_down, flow_right):
    from_above = jnp.concatenate([jnp.zeros_like(flow_down[:1]), flow_down[:-1]], 0)
    from_left = jnp.concatenate([jnp.zeros_like(flow_right[:, :1]), flow_right[:, :-1]], 1)
    return flow_down - from_above + flow_right - from_left

def shrink(moved_down, moved_right, threshold):
    magnitude = jnp.sqrt(moved_down * moved_down + moved_right * moved_right)
    factor = jnp.maximum(magnitude - threshold, 0.0) / jnp.maximum(magnitude, threshold)
    return (factor * moved_down, factor * moved_right)

def solve_pair(arrays, cost):
    source, flow_down, flow_right, potential = arrays
    primal_rate = jnp.full((), initial_step, jnp.float32)
    dual_rate = jnp.full((), initial_step, jnp.float32)
    spread_old = divergence(flow_down, flow_right)
    for iteration in range(ITERS):
        slope_down, slope_right = gradient(potential)
        new_down, new_right = shrink(flow_down + primal_rate * slope_down, flow_right + primal_rate * slope_right, primal_rate * cost)
        spread_new = divergence(new_down, new_right)
        new_potential = potential + dual_rate * (2.0 * spread_new - spread_old - source)
        if iteration + 1 < ITERS:
            diff_down = new_down - flow_down
            diff_right = new_right - flow_right
            primal_change = jnp.sum(diff_down * diff_down + diff_right * diff_right)
            change = new_potential - potential
            dual_change = jnp.sum(change * change)
            rescale = jnp.sqrt(jnp.sqrt((primal_change + epsilon) / (dual_change + epsilon)))
            primal_rate = primal_rate / rescale
            dual_rate = dual_rate * rescale
        flow_down, flow_right, potential, spread_old = (new_down, new_right, new_potential, spread_new)
    shortfall = spread_old - source
    residual = jnp.sum(shortfall * shortfall) / (NR * NC)
    return (flow_down, flow_right, potential, residual)

def reference(imbalance, flow, potential, cost):
    result_down, result_right, result_potential, residual = lax.map(partial(solve_pair, cost=cost), (imbalance, flow[0], flow[1], potential))
    return (jnp.stack([result_down, result_right]), result_potential, residual)
```

```python
import functools

import jax
import jax.numpy as jnp
from jax import lax
from jax.experimental import pallas as pl
from jax.experimental.pallas import tpu as pltpu
from jax.sharding import PartitionSpec as P

ITERS = 12
LANES = 128
SUBS = 8

initial_step = 0.35
epsilon = 1e-06
MESH = pl.DeviceIdType.MESH


def kernel(
    ny, nx,
    imb_hbm, flow_hbm, u_hbm, cost_hbm,
    flow_hbm_out, u_hbm_out, res_out,
    imb_in, flow_in, u_in, cost_in,
    A, B, U, E, Q, CH, GA, GB, IM, CO,
    tau_ref, sig_ref,
    row_send, col_send, row_recv, col_recv, corner_recv, msg_send, msg_recv,
    ext_row, ext_col, ext_row_in, ext_col_in, cost_row, cost_col, cost_row_in, cost_col_in,
    grow, gcol, slope_row, slope_col,
    halo_ssem, halo_rsem, msg_ssem, msg_rsem, ext_ssem, ext_rsem, in_sem, out_sem,
):
    G, T, _, C = A.shape
    n = ny * nx
    rows = T * SUBS
    gy, gx = lax.axis_index("gy"), lax.axis_index("gx")
    me = gy * nx + gx
    up, down, left, right = gy > 0, gy < ny - 1, gx > 0, gx < nx - 1
    f32 = jnp.float32
    K = C // LANES

    def piece(ref, k):
        return ref.at[(slice(None),) * (len(ref.shape) - 1) + (pl.ds(k * LANES, LANES),)]

    def fetch(i, g, k):
        if i == 0:
            return pltpu.make_async_copy(piece(cost_hbm, k), cost_in.at[k], in_sem.at[0, 0, k])
        if i == 1:
            return pltpu.make_async_copy(piece(u_hbm.at[g], k), u_in.at[k, g], in_sem.at[1, g, k])
        if i == 2:
            return pltpu.make_async_copy(
                flow_hbm.at[:, g, :, pl.ds(k * LANES, LANES)], flow_in.at[k, :, g], in_sem.at[2, g, k]
            )
        return pltpu.make_async_copy(piece(imb_hbm.at[g], k), imb_in.at[k, g], in_sem.at[3, g, k])

    def start_fetch(i, g):
        for k in range(K):
            fetch(i, g, k).start()

    def wait_fetch(i, g):
        for k in range(K):
            fetch(i, g, k).wait()

    half = ny // 2
    low = gy < half
    xs = [lax.rem(gx + d, nx) for d in range(nx)]
    order = sorted(range(nx), key=lambda d: -min(d, nx - d))
    places = [(jnp.where(low, ny - 1 - j, j), xs[d]) for j in range(half) for d in order]
    high = jnp.where(low, ny - 1 - gy, gy) - half
    for k in range(1, ny - half):
        y = half + lax.rem(high + k, ny - half)
        places += [(jnp.where(low, ny - 1 - y, y), xs[d]) for d in order]
    places += [(gy, xs[d]) for d in order if d]

    barrier = pltpu.get_barrier_semaphore()
    for where in places:
        pl.semaphore_signal(barrier, inc=1, device_id=where, device_id_type=MESH)

    start_fetch(0, 0)
    start_fetch(1, 0)
    start_fetch(2, 0)

    def later(g, c):
        start_fetch(1, g)
        start_fetch(2, g)
        return c

    lax.fori_loop(1, G, later, 0)

    def last(g, c):
        start_fetch(3, g)
        return c

    lax.fori_loop(0, G, last, 0)

    def gather(ref, *index):
        at = pl.ds(index[-1], SUBS, stride=T)
        return jnp.concatenate([ref[(k,) + index[:-1] + (at, slice(None))] for k in range(K)], axis=1)

    def scatter(ref, value, *index):
        at = pl.ds(index[-1], SUBS, stride=T)
        for k in range(K):
            ref[(k,) + index[:-1] + (at, slice(None))] = value[:, k * LANES:(k + 1) * LANES]

    def line(ref, *index):
        return jnp.concatenate([ref[(k,) + index[:-1] + (pl.ds(index[-1], 1), slice(None))] for k in range(K)], axis=1)

    lane = lax.broadcasted_iota(jnp.int32, (SUBS, LANES), 1)
    sub = lax.broadcasted_iota(jnp.int32, (SUBS, LANES), 0)
    subw = lax.broadcasted_iota(jnp.int32, (SUBS, C), 0)
    ones = jnp.ones((SUBS, LANES), f32)

    def wide(x):
        return jnp.concatenate([x] * K, axis=1)

    def row8(x):
        return jnp.broadcast_to(x, (SUBS, x.shape[1]))

    def turn_lanes(x, by):
        return pltpu.roll(x, by % LANES, 1) if by % LANES else x

    def to_left(x, entering):
        r = pltpu.roll(x, C - 1, 1)
        lanes = lax.broadcasted_iota(jnp.int32, entering.shape, 1)
        tail = jnp.where(lanes == LANES - 1, entering, r[:, C - LANES:])
        return jnp.concatenate([r[:, : C - LANES], tail], axis=1)

    def to_right(x, entering):
        r = pltpu.roll(x, 1, 1)
        head = jnp.where(lane == 0, entering, r[:, :LANES])
        return jnp.concatenate([head, r[:, LANES:]], axis=1)

    def pack_first(acc, v, t):
        return jnp.where(lane == t, turn_lanes(v, t), acc)

    def pack_last(acc, v, t):
        return jnp.where(lane == t, turn_lanes(v, t + 1), acc)

    def remote(src, dst, ssem, rsem, where):
        return pltpu.make_async_remote_copy(
            src_ref=src, dst_ref=dst, send_sem=ssem, recv_sem=rsem, device_id=where, device_id_type=MESH
        )

    def halos(slot, g):
        sems = lambda k: (halo_ssem.at[slot, k, g], halo_rsem.at[slot, k, g])
        head, tail = row_send.at[slot, 0, g], row_send.at[slot, 1, g]
        return [
            (up, down, remote(head, row_recv.at[slot, 0, g], *sems(0), (gy - 1, gx))),
            (down, up, remote(tail, row_recv.at[slot, 1, g], *sems(1), (gy + 1, gx))),
            (left, right, remote(col_send.at[slot, 0, g], col_recv.at[slot, 0, g], *sems(2), (gy, gx - 1))),
            (right, left, remote(col_send.at[slot, 1, g], col_recv.at[slot, 1, g], *sems(3), (gy, gx + 1))),
            (
                jnp.logical_and(down, left), jnp.logical_and(up, right),
                remote(tail.at[:, pl.ds(0, LANES)], corner_recv.at[slot, 0, g], *sems(4), (gy + 1, gx - 1)),
            ),
            (
                jnp.logical_and(up, right), jnp.logical_and(down, left),
                remote(head.at[:, pl.ds(C - LANES, LANES)], corner_recv.at[slot, 1, g], *sems(5), (gy - 1, gx + 1)),
            ),
        ]

    def extras(g):
        return [
            (down, up, remote(ext_row.at[g], ext_row_in.at[g], ext_ssem.at[0, g], ext_rsem.at[0, g], (gy + 1, gx))),
            (right, left, remote(ext_col.at[g], ext_col_in.at[g], ext_ssem.at[1, g], ext_rsem.at[1, g], (gy, gx + 1))),
        ]

    def prices():
        return [
            (down, up, remote(cost_row, cost_row_in, ext_ssem.at[0, G], ext_rsem.at[0, G], (gy + 1, gx))),
            (right, left, remote(cost_col, cost_col_in, ext_ssem.at[1, G], ext_rsem.at[1, G], (gy, gx + 1))),
        ]

    def start_all(copies):
        for ok_to, _, copy in copies:
            @pl.when(ok_to)
            def _(copy=copy):
                copy.start()

    def wait_all(copies):
        for ok_to, ok_from, copy in copies:
            @pl.when(ok_from)
            def _(copy=copy):
                copy.wait_recv()

            @pl.when(ok_to)
            def _(copy=copy):
                copy.wait_send()

    def send_message(slot, g, row):
        msg_send[slot, g] = row
        msg_recv[slot, g, me] = row
        for where in places:
            remote(
                msg_send.at[slot, g], msg_recv.at[slot, g, me], msg_ssem.at[slot, g], msg_rsem.at[slot, g], where
            ).start()

    def wait_message(slot, g):
        whole = msg_recv.at[slot, g, pl.ds(0, n - 1)]
        pltpu.make_async_copy(whole, whole, msg_rsem.at[slot, g]).wait()
        pltpu.make_async_copy(whole, whole, msg_ssem.at[slot, g]).wait()

    def totals(slot, g):
        parts = [msg_recv[slot, g, k] for k in range(n)]
        while len(parts) > 1:
            parts = [sum(parts[k + 1:k + 2], parts[k]) for k in range(0, len(parts), 2)]
        both = row8(parts[0])
        first = lane < LANES // 2
        return [
            jnp.sum(jnp.where(keep, both, 0.0), axis=1, keepdims=True) for keep in (first, jnp.logical_not(first))
        ]

    def fold(x, y):
        x, y = (sum((v[:, k * LANES:(k + 1) * LANES] for k in range(1, K)), v[:, :LANES]) for v in (x, y))
        first = lane < LANES // 2
        z = jnp.where(first, x, y) + pltpu.roll(jnp.where(first, y, x), LANES // 2, 1)
        for step in (4, 2, 1):
            z = z + pltpu.roll(z, step, 0)
        return z[0:1]


    def edges(g, c):
        wait_fetch(1, g)
        packs = [ones] * 4
        row_send[0, 0, g] = line(u_in, g, 0)
        row_send[0, 1, g] = line(u_in, g, rows - 1)
        for t in range(T):
            at = pl.ds(t, SUBS, stride=T)
            packs[0] = pack_first(packs[0], u_in[0, g, at, :], t)
            packs[1] = pack_last(packs[1], u_in[K - 1, g, at, :], t)
        wait_fetch(2, g)
        for t in range(T):
            at = pl.ds(t, SUBS, stride=T)
            packs[2] = pack_last(packs[2], flow_in[K - 1, 0, g, at, :], t)
            packs[3] = pack_last(packs[3], flow_in[K - 1, 1, g, at, :], t)
        col_send[0, 0, g] = packs[0]
        col_send[0, 1, g] = packs[1]
        for k in range(2):
            ext_col[g, k] = packs[2 + k]
            ext_row[g, k] = line(flow_in, k, g, rows - 1)
        return c

    wait_fetch(0, 0)
    pack = ones
    for t in range(T):
        CO[t] = gather(cost_in, t)
        pack = pack_last(pack, CO[t][:, C - LANES:], t)
    cost_col[...] = pack
    cost_row[...] = line(cost_in, rows - 1)
    lax.fori_loop(0, G, edges, 0)

    for missing, refs in (
        (jnp.logical_not(down), [row_recv.at[s, 0] for s in range(2)]),
        (jnp.logical_not(up), [row_recv.at[s, 1] for s in range(2)] + [ext_row_in]),
        (jnp.logical_not(right), [col_recv.at[s, 0] for s in range(2)]),
        (jnp.logical_not(left), [col_recv.at[s, 1] for s in range(2)] + [ext_col_in]),
        (jnp.logical_not(jnp.logical_and(up, right)), [corner_recv.at[s, 0] for s in range(2)]),
        (jnp.logical_not(jnp.logical_and(down, left)), [corner_recv.at[s, 1] for s in range(2)]),
    ):
        @pl.when(missing)
        def _(refs=refs):
            for ref in refs:
                ref[...] = jnp.zeros(ref.shape, f32)

    for missing, ref in ((jnp.logical_not(up), cost_row_in), (jnp.logical_not(left), cost_col_in)):
        @pl.when(missing)
        def _(ref=ref):
            ref[...] = jnp.ones(ref.shape, f32)

    pl.semaphore_wait(barrier, n - 1)
    start_all(prices())

    def announce(g, c):
        start_all(halos(0, g) + extras(g))
        return c

    lax.fori_loop(0, G, announce, 0)

    def load(g, c):
        wait_fetch(3, g)
        for t in range(T):
            A[g, t] = gather(flow_in, 0, g, t)
            B[g, t] = gather(flow_in, 1, g, t)
            U[g, t] = gather(u_in, g, t)
            IM[g, t] = gather(imb_in, g, t)
        return c

    lax.fori_loop(0, G, load, 0)

    def above_first(a_last, ghost):
        return jnp.where(subw == 0, row8(ghost), pltpu.roll(a_last, 1, 0))

    def divergence(t, a, above, b, gb):
        return ((a - above) + (b - to_right(b, turn_lanes(gb, -t))))

    def begin(g):
        wait_all(extras(g))
        for k in range(2):
            grow[g, k] = ext_row_in[g, k]
            gcol[g, k] = ext_col_in[g, k]
        gb = gcol[g, 1]
        for t in range(T):
            above = A[g, t - 1] if t else above_first(A[g, T - 1], grow[g, 0])
            E[g, t] = divergence(t, A[g, t], above, B[g, t], gb) + IM[g, t]

    def slopes(slot, g):
        wait_all(halos(slot, g))
        u = row_recv[slot, 1, g]
        u_right = to_left(u, turn_lanes(corner_recv[slot, 0, g], LANES - 1))
        zero = jnp.zeros_like(u)
        slope_row[g, 0] = jnp.where(up, row_send[slot, 0, g] - u, zero)
        slope_row[g, 1] = jnp.where(up, u_right - u, zero)
        u = col_recv[slot, 1, g]
        turn = turn_lanes(pltpu.roll(u, SUBS - 1, 0), T - 1)
        turn = jnp.where(sub == SUBS - 1, row8(turn_lanes(corner_recv[slot, 1, g], T)), turn)
        u_down = jnp.where(lane == T - 1, turn, turn_lanes(u, -1))
        zero = jnp.zeros_like(u)
        slope_col[g, 0] = jnp.where(left, u_down - u, zero)
        slope_col[g, 1] = jnp.where(left, col_send[slot, 0, g] - u, zero)
        below = row8(row_recv[slot, 0, g])
        beside = col_recv[slot, 0, g]
        first = u = U[g, 0]
        for t in range(T):
            if t < T - 1:
                u_down = U[g, t + 1]
            else:
                u_down = jnp.where(subw == SUBS - 1, below, pltpu.roll(first, SUBS - 1, 0))
            GA[g, t] = u_down - u
            GB[g, t] = to_left(u, turn_lanes(beside, LANES - 1 - t)) - u
            u = u_down

    def shrink(va, vb, t):
        f = jnp.maximum(1.0 - t * lax.rsqrt(va * va + vb * vb), 0.0)
        return f * va, f * vb

    def adapt(slot, g):
        wait_message(slot, g)
        primal, dual = (jnp.broadcast_to(v, (SUBS, LANES)) + epsilon for v in totals(slot, g))
        root = lax.rsqrt(primal) * (dual * lax.rsqrt(dual))
        s = lax.rsqrt(root)
        tau = tau_ref[g] * (root * s)
        sigma = sig_ref[g] * s
        tau_ref[g] = tau
        sig_ref[g] = sigma
        return tau, sigma

    def sweep(g, other, tau, sigma, closing):
        wtau, wsigma = wide(tau), wide(sigma)
        tau1 = wtau[0:1]
        ghost_a, ghost_b = shrink(
            grow[g, 0] + tau1 * slope_row[g, 0], grow[g, 1] + tau1 * slope_row[g, 1], tau1 * cost_row_in[...]
        )
        side_a, side_b = shrink(
            gcol[g, 0] + tau * slope_col[g, 0], gcol[g, 1] + tau * slope_col[g, 1], tau * cost_col_in[...]
        )
        grow[g, 0] = ghost_a
        grow[g, 1] = ghost_b
        gcol[g, 0] = side_a
        gcol[g, 1] = side_b
        acc_p = jnp.zeros((SUBS, C), f32)
        acc_d = jnp.zeros((SUBS, C), f32)

        def dual(t, a2, above, b2):
            nonlocal acc_d
            q2 = divergence(t, a2, above, b2, side_b)
            change = wsigma * ((q2 + q2) - E[g, t])
            CH[g, t] = change
            if closing:
                miss = q2 - IM[g, t]
                acc_d = acc_d + miss * miss
            else:
                Q[g, t] = q2
                acc_d = acc_d + change * change

        for t in range(T):
            a, b = A[g, t], B[g, t]
            a2, b2 = shrink(a + wtau * GA[g, t], b + wtau * GB[g, t], wtau * CO[t])
            if closing:
                scatter(flow_in, a2, 0, g, t)
                scatter(flow_in, b2, 1, g, t)
            else:
                A[g, t] = a2
                B[g, t] = b2
                da, db = a2 - a, b2 - b
                acc_p = acc_p + (da * da + db * db)
            if t:
                dual(t, a2, above, b2)
            else:
                a_first, b_first = a2, b2
            above = a2
        dual(0, a_first, above_first(above, ghost_a), b_first)
        send_message(other, g, fold(acc_p, acc_d))

    def settle(other, g):
        pack_f, pack_l = ones, ones
        for t in range(T):
            u2 = U[g, t] + CH[g, t]
            U[g, t] = u2
            E[g, t] = Q[g, t] + IM[g, t]
            pack_f = pack_first(pack_f, u2[:, :LANES], t)
            pack_l = pack_last(pack_l, u2[:, C - LANES:], t)
            if t == 0:
                row_send[other, 0, g] = u2[0:1]
            if t == T - 1:
                row_send[other, 1, g] = u2[SUBS - 1:]
        col_send[other, 0, g] = pack_f
        col_send[other, 1, g] = pack_l
        start_all(halos(other, g))

    wait_all(prices())

    def opening(g, c):
        begin(g)
        slopes(0, g)
        step = jnp.full((SUBS, LANES), initial_step, f32)
        tau_ref[g] = step
        sig_ref[g] = step
        sweep(g, 1, step, step, False)
        settle(1, g)
        return c

    lax.fori_loop(0, G, opening, 0)
    slopes(1, 0)

    def turn(i, c):
        slot = lax.rem(i, 2)
        other = 1 - slot

        def one(g, c):
            tau, sigma = adapt(slot, g)
            sweep(g, other, tau, sigma, False)
            settle(other, g)
            slopes(jnp.where(g == G - 1, other, slot), lax.rem(g + 1, G))
            return c

        return lax.fori_loop(0, G, one, c)

    lax.fori_loop(1, ITERS - 1, turn, 0)
    slot = (ITERS - 1) % 2

    def close(g, c):
        tau, sigma = adapt(slot, g)
        sweep(g, 1 - slot, tau, sigma, True)

        @pl.when(g < G - 1)
        def _():
            slopes(slot, g + 1)

        for t in range(T):
            scatter(u_in, U[g, t] + CH[g, t], g, t)
        return c

    lax.fori_loop(0, G, close, 0)
    results = [
        pltpu.make_async_copy(src.at[k], piece(dst, k), out_sem.at[i, k])
        for i, (src, dst) in enumerate(((flow_in, flow_hbm_out), (u_in, u_hbm_out)))
        for k in range(K)
    ]
    for copy in results:
        copy.start()
    cells = T * SUBS * C * n
    for g in range(G):
        wait_message(1 - slot, g)
        res_out[g] = jnp.broadcast_to(totals(1 - slot, g)[1], (SUBS, LANES)) / cells
    for copy in results:
        copy.wait()


def local(ny, nx, imbalance, flow, potential, cost):
    pairs, rows, cols = imbalance.shape
    T = rows // SUBS
    n = ny * nx
    assert rows % SUBS == 0 and cols % LANES == 0 and 4 <= T <= LANES and ny % 2 == 0
    G = pairs
    f32 = jnp.float32
    block = (pairs, T, SUBS, cols)
    packed = (SUBS, LANES)
    K = cols // LANES
    hbm = pl.BlockSpec(memory_space=pltpu.HBM)
    flow_out, u_out, res = pl.pallas_call(
        functools.partial(kernel, ny, nx),
        out_shape=(
            jax.ShapeDtypeStruct(flow.shape, f32),
            jax.ShapeDtypeStruct(potential.shape, f32),
            jax.ShapeDtypeStruct((G,) + packed, f32),
        ),
        in_specs=[hbm] * 4,
        out_specs=(hbm, hbm, pl.BlockSpec(memory_space=pltpu.VMEM)),
        scratch_shapes=[
            pltpu.VMEM((K, pairs, rows, LANES), f32), pltpu.VMEM((K, 2, pairs, rows, LANES), f32),
            pltpu.VMEM((K, pairs, rows, LANES), f32), pltpu.VMEM((K, rows, LANES), f32),
        ] + [pltpu.VMEM(block, f32)] * 9 + [
            pltpu.VMEM(block[1:], f32),
            pltpu.VMEM((G,) + packed, f32), pltpu.VMEM((G,) + packed, f32),
            pltpu.VMEM((2, 2, G, 1, cols), f32), pltpu.VMEM((2, 2, G) + packed, f32),
            pltpu.VMEM((2, 2, G, 1, cols), f32), pltpu.VMEM((2, 2, G) + packed, f32),
            pltpu.VMEM((2, 2, G, 1, LANES), f32),
            pltpu.VMEM((2, G, 1, LANES), f32), pltpu.VMEM((2, G, n, 1, LANES), f32),
            pltpu.VMEM((G, 2, 1, cols), f32), pltpu.VMEM((G, 2) + packed, f32),
            pltpu.VMEM((G, 2, 1, cols), f32), pltpu.VMEM((G, 2) + packed, f32),
            pltpu.VMEM((1, cols), f32), pltpu.VMEM(packed, f32),
            pltpu.VMEM((1, cols), f32), pltpu.VMEM(packed, f32),
            pltpu.VMEM((G, 2, 1, cols), f32), pltpu.VMEM((G, 2) + packed, f32),
            pltpu.VMEM((G, 2, 1, cols), f32), pltpu.VMEM((G, 2) + packed, f32),
            pltpu.SemaphoreType.DMA((2, 6, G)), pltpu.SemaphoreType.DMA((2, 6, G)),
            pltpu.SemaphoreType.DMA((2, G)), pltpu.SemaphoreType.DMA((2, G)),
            pltpu.SemaphoreType.DMA((2, G + 1)), pltpu.SemaphoreType.DMA((2, G + 1)),
            pltpu.SemaphoreType.DMA((4, G, K)), pltpu.SemaphoreType.DMA((2, K)),
        ],
        compiler_params=pltpu.CompilerParams(
            collective_id=0, has_side_effects=True, vmem_limit_bytes=48 * 1024 * 1024
        ),
    )(*(pltpu.with_memory_space_constraint(x, pltpu.HBM) for x in (imbalance, flow, potential, cost)))
    return flow_out, u_out, res[:, 0, 0]


def solution(mesh):
    placed = (P(None, "gy", "gx"), P(None, None, "gy", "gx"), P(None, "gy", "gx"), P("gy", "gx"))
    return jax.shard_map(
        functools.partial(local, mesh.shape["gy"], mesh.shape["gx"]),
        mesh=mesh,
        in_specs=placed,
        out_specs=(P(None, None, "gy", "gx"), P(None, "gy", "gx"), P()),
        check_vma=False,
    )
```

```python
import functools

import jax
import jax.numpy as jnp
from jax import lax
from jax.experimental import pallas as pl
from jax.experimental.pallas import tpu as pltpu
from jax.sharding import PartitionSpec as P

ITERS = 12
LANES = 128
SUBS = 8

initial_step = 0.35
epsilon = 1e-06
MESH = pl.DeviceIdType.MESH


def kernel(
    ny, nx,
    imb_hbm, flow_hbm, u_hbm, cost_hbm,
    flow_hbm_out, u_hbm_out, res_out,
    imb_in, flow_in, u_in, cost_in,
    A, B, U, E, W, GA, GB, IM, CO,
    tau_ref, sig_ref,
    row_send, col_send, row_recv, col_recv, corner_recv, msg_send, msg_recv,
    ext_row, ext_col, ext_row_in, ext_col_in, cost_row, cost_col, cost_row_in, cost_col_in,
    grow, gcol, slope_row, slope_col,
    res_row,
    halo_ssem, halo_rsem, msg_ssem, msg_rsem, ext_ssem, ext_rsem, in_sem, out_sem, plane_sem,
):
    G, T, _, C = A.shape
    n = ny * nx
    rows = T * SUBS
    gy, gx = lax.axis_index("gy"), lax.axis_index("gx")
    me = gy * nx + gx
    up, down, left, right = gy > 0, gy < ny - 1, gx > 0, gx < nx - 1
    f32 = jnp.float32
    K = C // LANES

    def piece(ref, k):
        return ref.at[(slice(None),) * (len(ref.shape) - 1) + (pl.ds(k * LANES, LANES),)]

    def fetch(i, g, k):
        if i == 0:
            return pltpu.make_async_copy(piece(cost_hbm, k), cost_in.at[k], in_sem.at[0, 0, k])
        if i == 1:
            return pltpu.make_async_copy(piece(u_hbm.at[g], k), u_in.at[k, g], in_sem.at[1, g, k])
        if i == 2:
            return pltpu.make_async_copy(
                flow_hbm.at[:, g, :, pl.ds(k * LANES, LANES)], flow_in.at[k, :, g], in_sem.at[2, g, k]
            )
        return pltpu.make_async_copy(piece(imb_hbm.at[g], k), imb_in.at[k, g], in_sem.at[3, g, k])

    def start_fetch(i, g):
        for k in range(K):
            fetch(i, g, k).start()

    def wait_fetch(i, g):
        for k in range(K):
            fetch(i, g, k).wait()

    half = ny // 2
    low = gy < half
    xs = [lax.rem(gx + d, nx) for d in range(nx)]
    order = sorted(range(nx), key=lambda d: -min(d, nx - d))
    places = [(jnp.where(low, ny - 1 - j, j), xs[d]) for j in range(half) for d in order]
    high = jnp.where(low, ny - 1 - gy, gy) - half
    for k in range(1, ny - half):
        y = half + lax.rem(high + k, ny - half)
        places += [(jnp.where(low, ny - 1 - y, y), xs[d]) for d in order]
    places += [(gy, xs[d]) for d in order if d]

    start_fetch(1, 0)
    start_fetch(0, 0)
    start_fetch(2, 0)
    barrier = pltpu.get_barrier_semaphore()

    def greet(where):
        pl.semaphore_signal(barrier, inc=1, device_id=where, device_id_type=MESH)

    odd = lax.rem(gy, 2)
    column = [(lax.rem(gy + 2 * k, ny), gx) for k in range(1, half)]
    mates = [(gy, xs[d]) for d in order if d] + [(gy + 1 - 2 * odd, xs[d]) for d in order]
    low_side, high_side = odd == 1, odd == 0
    outside = [
        (jnp.logical_and(low_side, down), (gy + 1, gx)),
        (jnp.logical_and(low_side, jnp.logical_and(down, left)), (gy + 1, gx - 1)),
        (jnp.logical_and(high_side, up), (gy - 1, gx)),
        (jnp.logical_and(high_side, jnp.logical_and(up, right)), (gy - 1, gx + 1)),
    ]
    for where in column + mates:
        greet(where)
    guests = len(column) + len(mates)
    for ok, where in outside:
        guests = guests + jnp.where(ok, 1, 0)

        @pl.when(ok)
        def _(where=where):
            greet(where)

    def later(g, c):
        start_fetch(1, g)
        start_fetch(2, g)
        return c

    lax.fori_loop(1, G, later, 0)

    def last(g, c):
        start_fetch(3, g)
        return c

    lax.fori_loop(0, G, last, 0)

    def gather(ref, *index):
        at = pl.ds(index[-1], SUBS, stride=T)
        return jnp.concatenate([ref[(k,) + index[:-1] + (at, slice(None))] for k in range(K)], axis=1)

    def scatter(ref, value, *index):
        at = pl.ds(index[-1], SUBS, stride=T)
        for k in range(K):
            ref[(k,) + index[:-1] + (at, slice(None))] = value[:, k * LANES:(k + 1) * LANES]

    def line(ref, *index):
        return jnp.concatenate([ref[(k,) + index[:-1] + (pl.ds(index[-1], 1), slice(None))] for k in range(K)], axis=1)

    lane = lax.broadcasted_iota(jnp.int32, (SUBS, LANES), 1)
    sub = lax.broadcasted_iota(jnp.int32, (SUBS, LANES), 0)
    subw = lax.broadcasted_iota(jnp.int32, (SUBS, C), 0)
    ones = jnp.ones((SUBS, LANES), f32)

    def wide(x):
        return jnp.concatenate([x] * K, axis=1)

    def row8(x):
        return jnp.broadcast_to(x, (SUBS, x.shape[1]))

    def turn_lanes(x, by):
        return pltpu.roll(x, by % LANES, 1) if by % LANES else x

    def to_left(x, entering):
        r = pltpu.roll(x, C - 1, 1)
        lanes = lax.broadcasted_iota(jnp.int32, entering.shape, 1)
        tail = jnp.where(lanes == LANES - 1, entering, r[:, C - LANES:])
        return jnp.concatenate([r[:, : C - LANES], tail], axis=1)

    def to_right(x, entering):
        r = pltpu.roll(x, 1, 1)
        head = jnp.where(lane == 0, entering, r[:, :LANES])
        return jnp.concatenate([head, r[:, LANES:]], axis=1)

    def pack_first(acc, v, t):
        return jnp.where(lane == t, turn_lanes(v, t), acc)

    def pack_last(acc, v, t):
        return jnp.where(lane == t, turn_lanes(v, t + 1), acc)

    def remote(src, dst, ssem, rsem, where):
        return pltpu.make_async_remote_copy(
            src_ref=src, dst_ref=dst, send_sem=ssem, recv_sem=rsem, device_id=where, device_id_type=MESH
        )

    def halos(slot, g):
        sems = lambda k: (halo_ssem.at[slot, k, g], halo_rsem.at[slot, k, g])
        head, tail = row_send.at[slot, 0, g], row_send.at[slot, 1, g]
        return [
            (up, down, remote(head, row_recv.at[slot, 0, g], *sems(0), (gy - 1, gx))),
            (down, up, remote(tail, row_recv.at[slot, 1, g], *sems(1), (gy + 1, gx))),
            (left, right, remote(col_send.at[slot, 0, g], col_recv.at[slot, 0, g], *sems(2), (gy, gx - 1))),
            (right, left, remote(col_send.at[slot, 1, g], col_recv.at[slot, 1, g], *sems(3), (gy, gx + 1))),
            (
                jnp.logical_and(down, left), jnp.logical_and(up, right),
                remote(tail.at[:, pl.ds(0, LANES)], corner_recv.at[slot, 0, g], *sems(4), (gy + 1, gx - 1)),
            ),
            (
                jnp.logical_and(up, right), jnp.logical_and(down, left),
                remote(head.at[:, pl.ds(C - LANES, LANES)], corner_recv.at[slot, 1, g], *sems(5), (gy - 1, gx + 1)),
            ),
        ]

    def extras(g):
        return [
            (down, up, remote(ext_row.at[g], ext_row_in.at[g], ext_ssem.at[0, g], ext_rsem.at[0, g], (gy + 1, gx))),
            (right, left, remote(ext_col.at[g], ext_col_in.at[g], ext_ssem.at[1, g], ext_rsem.at[1, g], (gy, gx + 1))),
        ]

    def prices():
        return [
            (down, up, remote(cost_row, cost_row_in, ext_ssem.at[0, G], ext_rsem.at[0, G], (gy + 1, gx))),
            (right, left, remote(cost_col, cost_col_in, ext_ssem.at[1, G], ext_rsem.at[1, G], (gy, gx + 1))),
        ]

    def start_all(copies):
        for ok_to, _, copy in copies:
            @pl.when(ok_to)
            def _(copy=copy):
                copy.start()

    def wait_all(copies):
        for ok_to, ok_from, copy in copies:
            @pl.when(ok_from)
            def _(copy=copy):
                copy.wait_recv()

            @pl.when(ok_to)
            def _(copy=copy):
                copy.wait_send()

    def send_message(slot, g, row, chores):
        msg_send[slot, g] = row
        msg_recv[slot, g, me] = row
        done = 0
        for k, where in enumerate(places):
            remote(
                msg_send.at[slot, g], msg_recv.at[slot, g, me], msg_ssem.at[slot, g], msg_rsem.at[slot, g], where
            ).start()
            while done * len(places) < k * len(chores):
                chores[done]()
                done += 1
        for chore in chores[done:]:
            chore()

    def wait_message(slot, g):
        whole = msg_recv.at[slot, g, pl.ds(0, n - 1)]
        pltpu.make_async_copy(whole, whole, msg_rsem.at[slot, g]).wait()
        pltpu.make_async_copy(whole, whole, msg_ssem.at[slot, g]).wait()

    def totals(slot, g):
        parts = [msg_recv[slot, g, k] for k in range(n)]
        while len(parts) > 1:
            parts = [sum(parts[k + 1:k + 2], parts[k]) for k in range(0, len(parts), 2)]
        both = row8(parts[0])
        first = lane < LANES // 2
        return [
            jnp.sum(jnp.where(keep, both, 0.0), axis=1, keepdims=True) for keep in (first, jnp.logical_not(first))
        ]

    def fold(x, y):
        x, y = (sum((v[:, k * LANES:(k + 1) * LANES] for k in range(1, K)), v[:, :LANES]) for v in (x, y))
        first = lane < LANES // 2
        z = jnp.where(first, x, y) + pltpu.roll(jnp.where(first, y, x), LANES // 2, 1)
        for step in (4, 2, 1):
            z = z + pltpu.roll(z, step, 0)
        return z[0:1]


    def edges(g, c):
        wait_fetch(1, g)
        packs = [ones] * 4
        row_send[0, 0, g] = line(u_in, g, 0)
        row_send[0, 1, g] = line(u_in, g, rows - 1)
        for t in range(T):
            at = pl.ds(t, SUBS, stride=T)
            packs[0] = pack_first(packs[0], u_in[0, g, at, :], t)
            packs[1] = pack_last(packs[1], u_in[K - 1, g, at, :], t)
        wait_fetch(2, g)
        for t in range(T):
            at = pl.ds(t, SUBS, stride=T)
            packs[2] = pack_last(packs[2], flow_in[K - 1, 0, g, at, :], t)
            packs[3] = pack_last(packs[3], flow_in[K - 1, 1, g, at, :], t)
        col_send[0, 0, g] = packs[0]
        col_send[0, 1, g] = packs[1]
        for k in range(2):
            ext_col[g, k] = packs[2 + k]
            ext_row[g, k] = line(flow_in, k, g, rows - 1)
        return c

    wait_fetch(0, 0)
    pack = ones
    for t in range(T):
        CO[t] = gather(cost_in, t)
        pack = pack_last(pack, CO[t][:, C - LANES:], t)
    cost_col[...] = pack
    cost_row[...] = line(cost_in, rows - 1)

    for missing, refs in (
        (jnp.logical_not(down), [row_recv.at[s, 0] for s in range(2)]),
        (jnp.logical_not(up), [row_recv.at[s, 1] for s in range(2)] + [ext_row_in]),
        (jnp.logical_not(right), [col_recv.at[s, 0] for s in range(2)]),
        (jnp.logical_not(left), [col_recv.at[s, 1] for s in range(2)] + [ext_col_in]),
        (jnp.logical_not(jnp.logical_and(up, right)), [corner_recv.at[s, 0] for s in range(2)]),
        (jnp.logical_not(jnp.logical_and(down, left)), [corner_recv.at[s, 1] for s in range(2)]),
    ):
        @pl.when(missing)
        def _(refs=refs):
            for ref in refs:
                ref[...] = jnp.zeros(ref.shape, f32)

    for missing, ref in ((jnp.logical_not(up), cost_row_in), (jnp.logical_not(left), cost_col_in)):
        @pl.when(missing)
        def _(ref=ref):
            ref[...] = jnp.ones(ref.shape, f32)

    edges(0, 0)
    pl.semaphore_wait(barrier, guests)
    for where in column:
        pl.semaphore_signal(plane_sem, inc=1, device_id=where, device_id_type=MESH)
    start_all(halos(0, 0) + extras(0) + prices())

    def announce(g, c):
        edges(g, c)
        start_all(halos(0, g) + extras(g))
        return c

    lax.fori_loop(1, G, announce, 0)

    no_lane = jnp.zeros((SUBS, LANES), f32)

    def above_first(a_last, ghost):
        return jnp.where(subw == 0, row8(ghost), pltpu.roll(a_last, 1, 0))

    def below_last(u_first):
        return jnp.where(subw == SUBS - 1, 0.0, pltpu.roll(u_first, SUBS - 1, 0))

    def load(g, c):
        wait_fetch(3, g)
        for t in range(T):
            A[g, t] = gather(flow_in, 0, g, t)
            B[g, t] = gather(flow_in, 1, g, t)
            U[g, t] = gather(u_in, g, t)
            IM[g, t] = gather(imb_in, g, t)
        for t in range(T):
            a, b, u = A[g, t], B[g, t], U[g, t]
            above = A[g, t - 1] if t else above_first(A[g, T - 1], jnp.zeros((1, C), f32))
            E[g, t] = ((a - above) + (b - to_right(b, no_lane))) + IM[g, t]
            GA[g, t] = (U[g, t + 1] if t < T - 1 else below_last(U[g, 0])) - u
            GB[g, t] = to_left(u, no_lane) - u
        return c

    lax.fori_loop(0, G, load, 0)
    pl.semaphore_wait(plane_sem, len(column))

    def divergence(t, a, above, b, gb):
        return ((a - above) + (b - to_right(b, turn_lanes(gb, -t))))

    def begin(g):
        wait_all(extras(g))
        for k in range(2):
            grow[g, k] = ext_row_in[g, k]
            gcol[g, k] = ext_col_in[g, k]
        gb = gcol[g, 1]
        E[g, 0] = E[g, 0] - jnp.where(subw == 0, row8(grow[g, 0]), 0.0)
        for t in range(T):
            E[g, t, :, :LANES] = E[g, t, :, :LANES] - jnp.where(lane == 0, turn_lanes(gb, -t), 0.0)

    def slopes(slot, g):
        wait_all(halos(slot, g))
        u = row_recv[slot, 1, g]
        u_right = to_left(u, turn_lanes(corner_recv[slot, 0, g], LANES - 1))
        zero = jnp.zeros_like(u)
        slope_row[g, 0] = jnp.where(up, row_send[slot, 0, g] - u, zero)
        slope_row[g, 1] = jnp.where(up, u_right - u, zero)
        u = col_recv[slot, 1, g]
        turn = turn_lanes(pltpu.roll(u, SUBS - 1, 0), T - 1)
        turn = jnp.where(sub == SUBS - 1, row8(turn_lanes(corner_recv[slot, 1, g], T)), turn)
        u_down = jnp.where(lane == T - 1, turn, turn_lanes(u, -1))
        zero = jnp.zeros_like(u)
        slope_col[g, 0] = jnp.where(left, u_down - u, zero)
        slope_col[g, 1] = jnp.where(left, col_send[slot, 0, g] - u, zero)
        GA[g, T - 1] = GA[g, T - 1] + jnp.where(subw == SUBS - 1, row8(row_recv[slot, 0, g]), 0.0)
        beside = col_recv[slot, 0, g]
        for t in range(T):
            entering = jnp.where(lane == LANES - 1, turn_lanes(beside, LANES - 1 - t), 0.0)
            GB[g, t, :, C - LANES:] = GB[g, t, :, C - LANES:] + entering

    def shrink(va, vb, t):
        f = jnp.maximum(1.0 - t * lax.rsqrt(va * va + vb * vb), 0.0)
        return f * va, f * vb

    def adapt(slot, g):
        wait_message(slot, g)
        sigma = sig_ref[g]
        primal, dual = (jnp.broadcast_to(v, (SUBS, LANES)) for v in totals(slot, g))
        primal = primal + epsilon
        dual = sigma * sigma * dual + epsilon
        root = lax.rsqrt(primal) * (dual * lax.rsqrt(dual))
        s = lax.rsqrt(root)
        tau = tau_ref[g] * (root * s)
        sigma = sigma * s
        tau_ref[g] = tau
        sig_ref[g] = sigma
        return tau, sigma

    def sweep(g, other, tau, closing, chores):
        wtau = wide(tau)
        tau1 = wtau[0:1]
        ghost_a, ghost_b = shrink(
            grow[g, 0] + tau1 * slope_row[g, 0], grow[g, 1] + tau1 * slope_row[g, 1], tau1 * cost_row_in[...]
        )
        side_a, side_b = shrink(
            gcol[g, 0] + tau * slope_col[g, 0], gcol[g, 1] + tau * slope_col[g, 1], tau * cost_col_in[...]
        )
        grow[g, 0] = ghost_a
        grow[g, 1] = ghost_b
        gcol[g, 0] = side_a
        gcol[g, 1] = side_b
        acc_p = jnp.zeros((SUBS, C), f32)
        acc_d = jnp.zeros((SUBS, C), f32)

        def dual(t, a2, above, b2):
            nonlocal acc_d
            q2 = divergence(t, a2, above, b2, side_b)
            w = (q2 + q2) - E[g, t]
            W[g, t] = w
            if closing:
                w = q2 - IM[g, t]
            acc_d = acc_d + w * w

        for t in range(T):
            a, b = A[g, t], B[g, t]
            a2, b2 = shrink(a + wtau * GA[g, t], b + wtau * GB[g, t], wtau * CO[t])
            if closing:
                scatter(flow_in, a2, 0, g, t)
                scatter(flow_in, b2, 1, g, t)
            else:
                A[g, t] = a2
                B[g, t] = b2
                da, db = a2 - a, b2 - b
                acc_p = acc_p + (da * da + db * db)
            if t:
                dual(t, a2, above, b2)
            else:
                a_first, b_first = a2, b2
            above = a2
        dual(0, a_first, above_first(above, ghost_a), b_first)
        send_message(other, g, fold(acc_p, acc_d), chores)

    def settle(other, g, sigma):
        pack_f, pack_l = ones, ones
        first = prev = None
        wsigma = wide(sigma)

        def chore(t):
            nonlocal pack_f, pack_l, first, prev
            w = W[g, t]
            u2 = U[g, t] + wsigma * w
            U[g, t] = u2
            E[g, t] = 0.5 * (w + E[g, t]) + IM[g, t]
            GB[g, t] = to_left(u2, no_lane) - u2
            pack_f = pack_first(pack_f, u2[:, :LANES], t)
            pack_l = pack_last(pack_l, u2[:, C - LANES:], t)
            if t == 0:
                row_send[other, 0, g] = u2[0:1]
                first = u2
            else:
                GA[g, t - 1] = u2 - prev
            if t == T - 1:
                row_send[other, 1, g] = u2[SUBS - 1:]
                GA[g, t] = below_last(first) - u2
            prev = u2

        def leave():
            col_send[other, 0, g] = pack_f
            col_send[other, 1, g] = pack_l
            start_all(halos(other, g))

        return [functools.partial(chore, t) for t in range(T)], leave

    wait_all(prices())

    def opening(g, c):
        begin(g)
        slopes(0, g)
        step = jnp.full((SUBS, LANES), initial_step, f32)
        tau_ref[g] = step
        sig_ref[g] = step
        chores, leave = settle(1, g, step)
        sweep(g, 1, step, False, chores)
        leave()
        return c

    lax.fori_loop(0, G, opening, 0)
    slopes(1, 0)

    def turn(i, c):
        slot = lax.rem(i, 2)
        other = 1 - slot

        def one(g, c):
            tau, sigma = adapt(slot, g)
            chores, leave = settle(other, g, sigma)
            sweep(g, other, tau, False, chores)
            leave()
            slopes(jnp.where(g == G - 1, other, slot), lax.rem(g + 1, G))
            return c

        return lax.fori_loop(0, G, one, c)

    lax.fori_loop(1, ITERS - 1, turn, 0)
    slot = (ITERS - 1) % 2

    def close(g, c):
        tau, sigma = adapt(slot, g)
        wsigma = wide(sigma)

        def chore(t):
            scatter(u_in, U[g, t] + wsigma * W[g, t], g, t)

        sweep(g, 1 - slot, tau, True, [functools.partial(chore, t) for t in range(T)])

        @pl.when(g < G - 1)
        def _():
            slopes(slot, g + 1)
        return c

    lax.fori_loop(0, G, close, 0)
    results = [
        pltpu.make_async_copy(src.at[k], piece(dst, k), out_sem.at[i, k])
        for i, (src, dst) in enumerate(((flow_in, flow_hbm_out), (u_in, u_hbm_out)))
        for k in range(K)
    ]
    for copy in results:
        copy.start()
    cells = T * SUBS * C * n
    row = ones
    for g in range(G):
        wait_message(1 - slot, g)
        row = jnp.where(lane == g, totals(1 - slot, g)[1] / cells, row)
    res_row[...] = row
    results.append(pltpu.make_async_copy(res_row, res_out, out_sem.at[2, 0]))
    results[-1].start()
    for copy in results:
        copy.wait()


def finish(flow_in, u_in, res_in, flow_out, u_out, res_out, row, short, sems):
    pairs = u_in.shape[0]
    pick = pltpu.make_async_copy(res_in, row, sems.at[0, 0])
    pick.start()
    copies = [pltpu.make_async_copy(u_in.at[g], u_out.at[g], sems.at[1, g]) for g in range(pairs)] + [
        pltpu.make_async_copy(flow_in.at[k, g], flow_out.at[k, g], sems.at[2 + k, g]) for k in range(2) for g in range(pairs)
    ]
    for copy in copies:
        copy.start()
    pick.wait()
    short[...] = row[0:1, 0:pairs]
    give = pltpu.make_async_copy(short, res_out, sems.at[0, 1])
    give.start()
    for copy in copies:
        copy.wait()
    give.wait()


def local(ny, nx, imbalance, flow, potential, cost):
    pairs, rows, cols = imbalance.shape
    T = rows // SUBS
    n = ny * nx
    assert rows % SUBS == 0 and cols % LANES == 0 and 4 <= T <= LANES and ny % 2 == 0
    G = pairs
    f32 = jnp.float32
    block = (pairs, T, SUBS, cols)
    packed = (SUBS, LANES)
    K = cols // LANES
    hbm = pl.BlockSpec(memory_space=pltpu.HBM)
    flow_out, u_out, res = pl.pallas_call(
        functools.partial(kernel, ny, nx),
        out_shape=(
            jax.ShapeDtypeStruct(flow.shape, f32),
            jax.ShapeDtypeStruct(potential.shape, f32),
            jax.ShapeDtypeStruct(packed, f32),
        ),
        in_specs=[hbm] * 4,
        out_specs=(hbm, hbm, hbm),
        scratch_shapes=[
            pltpu.VMEM((K, pairs, rows, LANES), f32), pltpu.VMEM((K, 2, pairs, rows, LANES), f32),
            pltpu.VMEM((K, pairs, rows, LANES), f32), pltpu.VMEM((K, rows, LANES), f32),
        ] + [pltpu.VMEM(block, f32)] * 8 + [
            pltpu.VMEM(block[1:], f32),
            pltpu.VMEM((G,) + packed, f32), pltpu.VMEM((G,) + packed, f32),
            pltpu.VMEM((2, 2, G, 1, cols), f32), pltpu.VMEM((2, 2, G) + packed, f32),
            pltpu.VMEM((2, 2, G, 1, cols), f32), pltpu.VMEM((2, 2, G) + packed, f32),
            pltpu.VMEM((2, 2, G, 1, LANES), f32),
            pltpu.VMEM((2, G, 1, LANES), f32), pltpu.VMEM((2, G, n, 1, LANES), f32),
            pltpu.VMEM((G, 2, 1, cols), f32), pltpu.VMEM((G, 2) + packed, f32),
            pltpu.VMEM((G, 2, 1, cols), f32), pltpu.VMEM((G, 2) + packed, f32),
            pltpu.VMEM((1, cols), f32), pltpu.VMEM(packed, f32),
            pltpu.VMEM((1, cols), f32), pltpu.VMEM(packed, f32),
            pltpu.VMEM((G, 2, 1, cols), f32), pltpu.VMEM((G, 2) + packed, f32),
            pltpu.VMEM((G, 2, 1, cols), f32), pltpu.VMEM((G, 2) + packed, f32),
            pltpu.VMEM(packed, f32),
            pltpu.SemaphoreType.DMA((2, 6, G)), pltpu.SemaphoreType.DMA((2, 6, G)),
            pltpu.SemaphoreType.DMA((2, G)), pltpu.SemaphoreType.DMA((2, G)),
            pltpu.SemaphoreType.DMA((2, G + 1)), pltpu.SemaphoreType.DMA((2, G + 1)),
            pltpu.SemaphoreType.DMA((4, G, K)), pltpu.SemaphoreType.DMA((3, K)), pltpu.SemaphoreType.REGULAR,
        ],
        compiler_params=pltpu.CompilerParams(
            collective_id=0, has_side_effects=True, vmem_limit_bytes=48 * 1024 * 1024
        ),
    )(*(pltpu.with_memory_space_constraint(x, pltpu.HBM) for x in (imbalance, flow, potential, cost)))
    anywhere = pl.BlockSpec(memory_space=pl.ANY)
    flow_out, u_out, res = pl.pallas_call(
        finish,
        out_shape=(
            jax.ShapeDtypeStruct(flow.shape, f32),
            jax.ShapeDtypeStruct(potential.shape, f32),
            jax.ShapeDtypeStruct((1, pairs), f32),
        ),
        in_specs=[anywhere] * 3,
        out_specs=(hbm, hbm, hbm),
        scratch_shapes=[pltpu.VMEM(packed, f32), pltpu.VMEM((1, pairs), f32), pltpu.SemaphoreType.DMA((4, max(pairs, 2)))],
    )(*(pltpu.with_memory_space_constraint(x, pltpu.VMEM) for x in (flow_out, u_out, res)))
    return flow_out, u_out, res.reshape(pairs)


def solution(mesh):
    placed = (P(None, "gy", "gx"), P(None, None, "gy", "gx"), P(None, "gy", "gx"), P("gy", "gx"))
    return jax.shard_map(
        functools.partial(local, mesh.shape["gy"], mesh.shape["gx"]),
        mesh=mesh,
        in_specs=placed,
        out_specs=(P(None, None, "gy", "gx"), P(None, "gy", "gx"), P()),
        check_vma=False,
    )
```

```python
import functools
import itertools

import jax
import jax.numpy as jnp
from jax import lax
from jax.experimental import pallas as pl
from jax.experimental.pallas import tpu as pltpu
from jax.sharding import PartitionSpec as P

ITERS = 12
LANES = 128
SUBS = 8

initial_step = 0.35
epsilon = 1e-06
MESH = pl.DeviceIdType.MESH


def kernel(
    ny, nx,
    imb_hbm, flow_hbm, u_hbm, cost_hbm,
    flow_hbm_out, u_hbm_out, res_out,
    imb_in, flow_in, u_in, cost_in,
    A, B, U, E, W, GA, GB, IM, CO,
    tau_ref, sig_ref,
    row_send, col_send, row_recv, col_recv, corner_recv, msg_send, msg_recv,
    ext_row, ext_col, ext_row_in, ext_col_in, cost_row, cost_col, cost_row_in, cost_col_in,
    grow, gcol, slope_row, slope_col,
    res_row, spare,
    halo_ssem, halo_rsem, msg_ssem, msg_rsem, ext_ssem, ext_rsem, in_sem, out_sem, plane_sem,
):
    G, T, _, C = A.shape
    n = ny * nx
    rows = T * SUBS
    gy, gx = lax.axis_index("gy"), lax.axis_index("gx")
    me = gy * nx + gx
    up, down, left, right = gy > 0, gy < ny - 1, gx > 0, gx < nx - 1
    f32 = jnp.float32
    K = C // LANES

    def piece(ref, k):
        return ref.at[(slice(None),) * (len(ref.shape) - 1) + (pl.ds(k * LANES, LANES),)]

    def start_fetch(i, g):
        for k in range(K):
            at = pl.ds(k * LANES, LANES)
            src, dst = (
                (cost_hbm.at[:, at], cost_in.at[k]), (u_hbm.at[g, :, at], u_in.at[k, g]),
                (flow_hbm.at[:, g, :, at], flow_in.at[k, :, g]), (imb_hbm.at[:, :, at], imb_in.at[k]),
            )[i]
            pltpu.make_async_copy(src, dst, in_sem.at[i, g]).start()

    def wait_fetch(i, g):
        whole = (cost_in, u_in.at[:, g], flow_in.at[:, :, g], imb_in)[i]
        pltpu.make_async_copy(whole, whole, in_sem.at[i, g]).wait()

    half = ny // 2
    low = gy < half
    xs = [lax.rem(gx + d, nx) for d in range(nx)]
    order = sorted(range(nx), key=lambda d: -min(d, nx - d))
    places = [(jnp.where(low, ny - 1 - j, j), xs[d]) for j in range(half) for d in order]
    high = jnp.where(low, ny - 1 - gy, gy) - half
    for k in range(1, ny - half):
        y = half + lax.rem(high + k, ny - half)
        places += [(jnp.where(low, ny - 1 - y, y), xs[d]) for d in order]
    places += [(gy, xs[d]) for d in order if d]

    start_fetch(1, 0)
    start_fetch(0, 0)
    start_fetch(2, 0)
    barrier = pltpu.get_barrier_semaphore()

    def greet(where):
        pl.semaphore_signal(barrier, inc=1, device_id=where, device_id_type=MESH)

    odd = lax.rem(gy, 2)
    column = [(lax.rem(gy + 2 * k, ny), gx) for k in range(1, half)]
    mates = [(gy, xs[d]) for d in order if d] + [(gy + 1 - 2 * odd, xs[d]) for d in order]
    low_side, high_side = odd == 1, odd == 0
    outside = [
        (jnp.logical_and(low_side, down), (gy + 1, gx)),
        (jnp.logical_and(low_side, jnp.logical_and(down, left)), (gy + 1, gx - 1)),
        (jnp.logical_and(high_side, up), (gy - 1, gx)),
        (jnp.logical_and(high_side, jnp.logical_and(up, right)), (gy - 1, gx + 1)),
    ]
    for where in column + mates:
        greet(where)
    guests = len(column) + len(mates)
    for ok, where in outside:
        guests = guests + jnp.where(ok, 1, 0)

        @pl.when(ok)
        def _(where=where):
            greet(where)

    def later(g, c):
        start_fetch(1, g)
        start_fetch(2, g)
        return c

    lax.fori_loop(1, G, later, 0)

    start_fetch(3, 0)

    def gather(ref, *index):
        at = pl.ds(index[-1], SUBS, stride=T)
        return jnp.concatenate([ref[(k,) + index[:-1] + (at, slice(None))] for k in range(K)], axis=1)

    def scatter(ref, value, *index):
        at = pl.ds(index[-1], SUBS, stride=T)
        for k in range(K):
            ref[(k,) + index[:-1] + (at, slice(None))] = value[:, k * LANES:(k + 1) * LANES]

    def line(ref, *index):
        return jnp.concatenate([ref[(k,) + index[:-1] + (pl.ds(index[-1], 1), slice(None))] for k in range(K)], axis=1)

    lane = lax.broadcasted_iota(jnp.int32, (SUBS, LANES), 1)
    sub = lax.broadcasted_iota(jnp.int32, (SUBS, LANES), 0)
    subw = lax.broadcasted_iota(jnp.int32, (SUBS, C), 0)
    ones = jnp.ones((SUBS, LANES), f32)

    def wide(x):
        return jnp.concatenate([x] * K, axis=1)

    def row8(x):
        return jnp.broadcast_to(x, (SUBS, x.shape[1]))

    def turn_lanes(x, by):
        return pltpu.roll(x, by % LANES, 1) if by % LANES else x

    def to_left(x, entering):
        r = pltpu.roll(x, C - 1, 1)
        lanes = lax.broadcasted_iota(jnp.int32, entering.shape, 1)
        tail = jnp.where(lanes == LANES - 1, entering, r[:, C - LANES:])
        return jnp.concatenate([r[:, : C - LANES], tail], axis=1)

    def to_right(x, entering):
        r = pltpu.roll(x, 1, 1)
        head = jnp.where(lane == 0, entering, r[:, :LANES])
        return jnp.concatenate([head, r[:, LANES:]], axis=1)

    def pack_first(acc, v, t):
        return jnp.where(lane == t, turn_lanes(v, t), acc)

    def pack_last(acc, v, t):
        return jnp.where(lane == t, turn_lanes(v, t + 1), acc)

    def remote(src, dst, ssem, rsem, where):
        return pltpu.make_async_remote_copy(
            src_ref=src, dst_ref=dst, send_sem=ssem, recv_sem=rsem, device_id=where, device_id_type=MESH
        )

    def halos(slot, g):
        sems = (halo_ssem.at[g], halo_rsem.at[slot, g])
        head, tail = row_send.at[slot, 0, g], row_send.at[slot, 1, g]
        return [
            (jnp.logical_and(down, left), remote(tail.at[:, pl.ds(0, LANES)], corner_recv.at[slot, 0, g], *sems, (gy + 1, gx - 1))),
            (jnp.logical_and(up, right), remote(head.at[:, pl.ds(C - LANES, LANES)], corner_recv.at[slot, 1, g], *sems, (gy - 1, gx + 1))),
            (up, remote(head, row_recv.at[slot, 0, g], *sems, (gy - 1, gx))),
            (down, remote(tail, row_recv.at[slot, 1, g], *sems, (gy + 1, gx))),
            (left, remote(col_send.at[slot, 0, g], col_recv.at[slot, 0, g], *sems, (gy, gx - 1))),
            (right, remote(col_send.at[slot, 1, g], col_recv.at[slot, 1, g], *sems, (gy, gx + 1))),
        ]

    def extras(g):
        sems = (ext_ssem.at[g], ext_rsem.at[g])
        return [
            (down, remote(ext_row.at[g], ext_row_in.at[g], *sems, (gy + 1, gx))),
            (right, remote(ext_col.at[g], ext_col_in.at[g], *sems, (gy, gx + 1))),
        ]

    def prices():
        sems = (ext_ssem.at[G], ext_rsem.at[G])
        return [
            (down, remote(cost_row, cost_row_in, *sems, (gy + 1, gx))),
            (right, remote(cost_col, cost_col_in, *sems, (gy, gx + 1))),
        ]

    def start_all(copies):
        for ok, copy in copies:
            @pl.when(ok)
            def _(copy=copy):
                copy.start()

    sides = [c for c in itertools.product((0, 1), repeat=4) if (c[0] or c[1]) and (c[2] or c[3])]

    def lies(case):
        flags = [f if has else jnp.logical_not(f) for f, has in zip((up, down, left, right), case)]
        return functools.reduce(jnp.logical_and, flags)

    def wait_rows(sem, count):
        totals_of = {}
        for case in sides:
            totals_of.setdefault(count(*case), []).append(case)
        for total, cases in totals_of.items():
            if total:
                @pl.when(functools.reduce(jnp.logical_or, [lies(case) for case in cases]))
                def _(total=total):
                    whole = spare.at[pl.ds(0, total)]
                    pltpu.make_async_copy(whole, whole, sem).wait()

    def wait_halos(slot, g):
        count = lambda u, d, l, r: K * (u + d) + SUBS * (l + r) + u * r + d * l
        wait_rows(halo_rsem.at[slot, g], count)
        wait_rows(halo_ssem.at[g], count)

    def wait_edges(k, parts):
        wait_rows(ext_rsem.at[k], lambda u, d, l, r: parts * (K * u + SUBS * l))
        wait_rows(ext_ssem.at[k], lambda u, d, l, r: parts * (K * d + SUBS * r))

    def send_message(slot, g, rows, chores):
        for k, row in enumerate(rows):
            msg_send[slot, g, k:k + 1] = row
            msg_recv[slot, g, me, k:k + 1] = row
        for where in places:
            remote(
                msg_send.at[slot, g], msg_recv.at[slot, g, me], msg_ssem.at[g], msg_rsem.at[slot, g], where
            ).start()
        for chore in chores:
            chore()

    def wait_message(slot, g):
        whole = msg_recv.at[slot, g, pl.ds(0, n - 1)]
        pltpu.make_async_copy(whole, whole, msg_rsem.at[slot, g]).wait()
        pltpu.make_async_copy(whole, whole, msg_ssem.at[g]).wait()

    def totals(slot, g):
        parts = [msg_recv[slot, g, k] for k in range(n)]
        while len(parts) > 1:
            parts = [sum(parts[k + 1:k + 2], parts[k]) for k in range(0, len(parts), 2)]
        return [jnp.sum(row8(parts[0][k:k + 1]), axis=1, keepdims=True) for k in range(2)]

    def fold(x, y):
        x, y = (sum((v[:, k * LANES:(k + 1) * LANES] for k in range(1, K)), v[:, :LANES]) for v in (x, y))
        half = SUBS // 2
        z = jnp.where(sub < half, x + pltpu.roll(x, half, 0), y + pltpu.roll(y, half, 0))
        z = z + pltpu.roll(z, 1, 0)
        z = z + pltpu.roll(z, 2, 0)
        return z[half - 1:half], z[SUBS - 1:]


    def edges(g, c):
        wait_fetch(1, g)
        packs = [ones] * 4
        row_send[0, 0, g] = line(u_in, g, 0)
        row_send[0, 1, g] = line(u_in, g, rows - 1)
        for t in range(T):
            at = pl.ds(t, SUBS, stride=T)
            packs[0] = pack_first(packs[0], u_in[0, g, at, :], t)
            packs[1] = pack_last(packs[1], u_in[K - 1, g, at, :], t)
        wait_fetch(2, g)
        for t in range(T):
            at = pl.ds(t, SUBS, stride=T)
            packs[2] = pack_last(packs[2], flow_in[K - 1, 0, g, at, :], t)
            packs[3] = pack_last(packs[3], flow_in[K - 1, 1, g, at, :], t)
        col_send[0, 0, g] = packs[0]
        col_send[0, 1, g] = packs[1]
        for k in range(2):
            ext_col[g, k] = packs[2 + k]
            ext_row[g, k] = line(flow_in, k, g, rows - 1)
        return c

    wait_fetch(0, 0)
    pack = ones
    for t in range(T):
        CO[t] = gather(cost_in, t)
        pack = pack_last(pack, CO[t][:, C - LANES:], t)
    cost_col[...] = pack
    cost_row[...] = line(cost_in, rows - 1)

    for missing, refs in (
        (jnp.logical_not(down), [row_recv.at[s, 0] for s in range(2)]),
        (jnp.logical_not(up), [row_recv.at[s, 1] for s in range(2)] + [ext_row_in]),
        (jnp.logical_not(right), [col_recv.at[s, 0] for s in range(2)]),
        (jnp.logical_not(left), [col_recv.at[s, 1] for s in range(2)] + [ext_col_in]),
        (jnp.logical_not(jnp.logical_and(up, right)), [corner_recv.at[s, 0] for s in range(2)]),
        (jnp.logical_not(jnp.logical_and(down, left)), [corner_recv.at[s, 1] for s in range(2)]),
    ):
        @pl.when(missing)
        def _(refs=refs):
            for ref in refs:
                ref[...] = jnp.zeros(ref.shape, f32)

    for missing, ref in ((jnp.logical_not(up), cost_row_in), (jnp.logical_not(left), cost_col_in)):
        @pl.when(missing)
        def _(ref=ref):
            ref[...] = jnp.ones(ref.shape, f32)

    edges(0, 0)
    pl.semaphore_wait(barrier, guests)
    for where in column:
        pl.semaphore_signal(plane_sem, inc=1, device_id=where, device_id_type=MESH)
    start_all(halos(0, 0) + extras(0) + prices())

    def announce(g, c):
        edges(g, c)
        start_all(halos(0, g) + extras(g))
        return c

    lax.fori_loop(1, G, announce, 0)

    no_lane = jnp.zeros((SUBS, LANES), f32)

    def above_first(a_last, ghost):
        return jnp.where(subw == 0, row8(ghost), pltpu.roll(a_last, 1, 0))

    def below_last(u_first):
        return jnp.where(subw == SUBS - 1, 0.0, pltpu.roll(u_first, SUBS - 1, 0))

    wait_fetch(3, 0)

    def load(g, c):
        for t in range(T):
            A[g, t] = gather(flow_in, 0, g, t)
            B[g, t] = gather(flow_in, 1, g, t)
            U[g, t] = gather(u_in, g, t)
            IM[g, t] = gather(imb_in, g, t)
        for t in range(T):
            a, b, u = A[g, t], B[g, t], U[g, t]
            above = A[g, t - 1] if t else above_first(A[g, T - 1], jnp.zeros((1, C), f32))
            E[g, t] = ((a - above) + (b - to_right(b, no_lane))) + IM[g, t]
            GA[g, t] = (U[g, t + 1] if t < T - 1 else below_last(U[g, 0])) - u
            GB[g, t] = to_left(u, no_lane) - u
        return c

    lax.fori_loop(0, G, load, 0)
    pl.semaphore_wait(plane_sem, len(column))

    def divergence(t, a, above, b, gb):
        return ((a - above) + (b - to_right(b, turn_lanes(gb, -t))))

    def begin(g):
        wait_edges(g, 2)
        for k in range(2):
            grow[g, k] = ext_row_in[g, k]
            gcol[g, k] = ext_col_in[g, k]
        gb = gcol[g, 1]
        E[g, 0] = E[g, 0] - jnp.where(subw == 0, row8(grow[g, 0]), 0.0)
        for t in range(T):
            E[g, t, :, :LANES] = E[g, t, :, :LANES] - jnp.where(lane == 0, turn_lanes(gb, -t), 0.0)

    def slopes(slot, g):
        wait_halos(slot, g)
        u = row_recv[slot, 1, g]
        u_right = to_left(u, turn_lanes(corner_recv[slot, 0, g], LANES - 1))
        zero = jnp.zeros_like(u)
        slope_row[g, 0] = jnp.where(up, row_send[slot, 0, g] - u, zero)
        slope_row[g, 1] = jnp.where(up, u_right - u, zero)
        u = col_recv[slot, 1, g]
        turn = turn_lanes(pltpu.roll(u, SUBS - 1, 0), T - 1)
        turn = jnp.where(sub == SUBS - 1, row8(turn_lanes(corner_recv[slot, 1, g], T)), turn)
        u_down = jnp.where(lane == T - 1, turn, turn_lanes(u, -1))
        zero = jnp.zeros_like(u)
        slope_col[g, 0] = jnp.where(left, u_down - u, zero)
        slope_col[g, 1] = jnp.where(left, col_send[slot, 0, g] - u, zero)
        GA[g, T - 1] = GA[g, T - 1] + jnp.where(subw == SUBS - 1, row8(row_recv[slot, 0, g]), 0.0)
        beside = col_recv[slot, 0, g]
        for t in range(T):
            entering = jnp.where(lane == LANES - 1, turn_lanes(beside, LANES - 1 - t), 0.0)
            GB[g, t, :, C - LANES:] = GB[g, t, :, C - LANES:] + entering

    def shrink(va, vb, t):
        f = jnp.maximum(1.0 - t * lax.rsqrt(va * va + vb * vb), 0.0)
        return f * va, f * vb

    def adapt(slot, g):
        wait_message(slot, g)
        sigma = sig_ref[g]
        primal, dual = (jnp.broadcast_to(v, (SUBS, LANES)) for v in totals(slot, g))
        primal = primal + epsilon
        dual = sigma * sigma * dual + epsilon
        root = lax.rsqrt(primal) * (dual * lax.rsqrt(dual))
        s = lax.rsqrt(root)
        tau = tau_ref[g] * (root * s)
        sigma = sigma * s
        tau_ref[g] = tau
        sig_ref[g] = sigma
        return tau, sigma

    def sweep(g, other, tau, closing, chores):
        wtau = wide(tau)
        tau1 = wtau[0:1]
        ghost_a, ghost_b = shrink(
            grow[g, 0] + tau1 * slope_row[g, 0], grow[g, 1] + tau1 * slope_row[g, 1], tau1 * cost_row_in[...]
        )
        side_a, side_b = shrink(
            gcol[g, 0] + tau * slope_col[g, 0], gcol[g, 1] + tau * slope_col[g, 1], tau * cost_col_in[...]
        )
        grow[g, 0] = ghost_a
        grow[g, 1] = ghost_b
        gcol[g, 0] = side_a
        gcol[g, 1] = side_b
        acc_p = jnp.zeros((SUBS, C), f32)
        acc_d = jnp.zeros((SUBS, C), f32)

        def dual(t, a2, above, b2):
            nonlocal acc_d
            q2 = divergence(t, a2, above, b2, side_b)
            w = (q2 + q2) - E[g, t]
            W[g, t] = w
            if closing:
                w = q2 - IM[g, t]
            acc_d = acc_d + w * w

        for t in range(T):
            a, b = A[g, t], B[g, t]
            a2, b2 = shrink(a + wtau * GA[g, t], b + wtau * GB[g, t], wtau * CO[t])
            if closing:
                scatter(flow_in, a2, 0, g, t)
                scatter(flow_in, b2, 1, g, t)
            else:
                A[g, t] = a2
                B[g, t] = b2
                da, db = a2 - a, b2 - b
                acc_p = acc_p + (da * da + db * db)
            if t:
                dual(t, a2, above, b2)
            else:
                a_first, b_first = a2, b2
            above = a2
        dual(0, a_first, above_first(above, ghost_a), b_first)
        send_message(other, g, fold(acc_p, acc_d), chores)

    def settle(other, g, sigma):
        pack_f, pack_l = ones, ones
        first = prev = None
        wsigma = wide(sigma)

        def chore(t):
            nonlocal pack_f, pack_l, first, prev
            w = W[g, t]
            u2 = U[g, t] + wsigma * w
            U[g, t] = u2
            E[g, t] = 0.5 * (w + E[g, t]) + IM[g, t]
            GB[g, t] = to_left(u2, no_lane) - u2
            pack_f = pack_first(pack_f, u2[:, :LANES], t)
            pack_l = pack_last(pack_l, u2[:, C - LANES:], t)
            if t == 0:
                row_send[other, 0, g] = u2[0:1]
                first = u2
            else:
                GA[g, t - 1] = u2 - prev
            if t == T - 1:
                row_send[other, 1, g] = u2[SUBS - 1:]
                GA[g, t] = below_last(first) - u2
            prev = u2

        def leave():
            col_send[other, 0, g] = pack_f
            col_send[other, 1, g] = pack_l
            start_all(halos(other, g))

        return [functools.partial(chore, t) for t in range(T)], leave

    wait_edges(G, 1)

    def opening(g, c):
        begin(g)
        slopes(0, g)
        step = jnp.full((SUBS, LANES), initial_step, f32)
        tau_ref[g] = step
        sig_ref[g] = step
        chores, leave = settle(1, g, step)
        sweep(g, 1, step, False, chores)
        leave()
        return c

    lax.fori_loop(0, G, opening, 0)
    slopes(1, 0)

    def turn(i, c):
        slot = lax.rem(i, 2)
        other = 1 - slot

        def one(g, c):
            tau, sigma = adapt(slot, g)
            chores, leave = settle(other, g, sigma)
            sweep(g, other, tau, False, chores)
            leave()
            slopes(jnp.where(g == G - 1, other, slot), lax.rem(g + 1, G))
            return c

        return lax.fori_loop(0, G, one, c)

    lax.fori_loop(1, ITERS - 1, turn, 0)
    slot = (ITERS - 1) % 2

    def close(g, c):
        tau, sigma = adapt(slot, g)
        wsigma = wide(sigma)

        def chore(t):
            scatter(u_in, U[g, t] + wsigma * W[g, t], g, t)

        sweep(g, 1 - slot, tau, True, [functools.partial(chore, t) for t in range(T)])

        @pl.when(g < G - 1)
        def _():
            slopes(slot, g + 1)
        return c

    lax.fori_loop(0, G, close, 0)
    results = [
        pltpu.make_async_copy(src.at[k], piece(dst, k), out_sem.at[i])
        for i, (src, dst) in enumerate(((flow_in, flow_hbm_out), (u_in, u_hbm_out)))
        for k in range(K)
    ]
    for copy in results:
        copy.start()
    cells = T * SUBS * C * n
    row = ones
    for g in range(G):
        wait_message(1 - slot, g)
        row = jnp.where(lane == g, totals(1 - slot, g)[1] / cells, row)
    res_row[...] = row
    give = pltpu.make_async_copy(res_row, res_out, out_sem.at[2])
    give.start()
    for i, whole in enumerate((flow_hbm_out, u_hbm_out)):
        pltpu.make_async_copy(whole, whole, out_sem.at[i]).wait()
    give.wait()


def finish(flow_in, u_in, res_in, flow_out, u_out, res_out, row, short, sems):
    pick = pltpu.make_async_copy(res_in, row, sems.at[0])
    pick.start()
    copies = [pltpu.make_async_copy(u_in, u_out, sems.at[1]), pltpu.make_async_copy(flow_in, flow_out, sems.at[2])]
    for copy in copies:
        copy.start()
    pick.wait()
    short[...] = row[0:1, 0:short.shape[1]]
    give = pltpu.make_async_copy(short, res_out, sems.at[0])
    give.start()
    for copy in copies:
        copy.wait()
    give.wait()


def local(ny, nx, imbalance, flow, potential, cost):
    pairs, rows, cols = imbalance.shape
    T = rows // SUBS
    n = ny * nx
    assert rows % SUBS == 0 and cols % LANES == 0 and 4 <= T < LANES and ny % 2 == 0 and nx > 1
    assert pairs <= LANES
    G = pairs
    f32 = jnp.float32
    block = (pairs, T, SUBS, cols)
    packed = (SUBS, LANES)
    K = cols // LANES
    hbm = pl.BlockSpec(memory_space=pltpu.HBM)
    flow_out, u_out, res = pl.pallas_call(
        functools.partial(kernel, ny, nx),
        out_shape=(
            jax.ShapeDtypeStruct(flow.shape, f32),
            jax.ShapeDtypeStruct(potential.shape, f32),
            jax.ShapeDtypeStruct(packed, f32),
        ),
        in_specs=[hbm] * 4,
        out_specs=(hbm, hbm, hbm),
        scratch_shapes=[
            pltpu.VMEM((K, pairs, rows, LANES), f32), pltpu.VMEM((K, 2, pairs, rows, LANES), f32),
            pltpu.VMEM((K, pairs, rows, LANES), f32), pltpu.VMEM((K, rows, LANES), f32),
        ] + [pltpu.VMEM(block, f32)] * 8 + [
            pltpu.VMEM(block[1:], f32),
            pltpu.VMEM((G,) + packed, f32), pltpu.VMEM((G,) + packed, f32),
            pltpu.VMEM((2, 2, G, 1, cols), f32), pltpu.VMEM((2, 2, G) + packed, f32),
            pltpu.VMEM((2, 2, G, 1, cols), f32), pltpu.VMEM((2, 2, G) + packed, f32),
            pltpu.VMEM((2, 2, G, 1, LANES), f32),
            pltpu.VMEM((2, G, 2, LANES), f32), pltpu.VMEM((2, G, n, 2, LANES), f32),
            pltpu.VMEM((G, 2, 1, cols), f32), pltpu.VMEM((G, 2) + packed, f32),
            pltpu.VMEM((G, 2, 1, cols), f32), pltpu.VMEM((G, 2) + packed, f32),
            pltpu.VMEM((1, cols), f32), pltpu.VMEM(packed, f32),
            pltpu.VMEM((1, cols), f32), pltpu.VMEM(packed, f32),
            pltpu.VMEM((G, 2, 1, cols), f32), pltpu.VMEM((G, 2) + packed, f32),
            pltpu.VMEM((G, 2, 1, cols), f32), pltpu.VMEM((G, 2) + packed, f32),
            pltpu.VMEM(packed, f32), pltpu.VMEM((2 * K + 2 * SUBS + 2, 1, LANES), f32),
            pltpu.SemaphoreType.DMA((G,)), pltpu.SemaphoreType.DMA((2, G)),
            pltpu.SemaphoreType.DMA((G,)), pltpu.SemaphoreType.DMA((2, G)),
            pltpu.SemaphoreType.DMA((G + 1,)), pltpu.SemaphoreType.DMA((G + 1,)),
            pltpu.SemaphoreType.DMA((4, G)), pltpu.SemaphoreType.DMA((3,)), pltpu.SemaphoreType.REGULAR,
        ],
        compiler_params=pltpu.CompilerParams(
            collective_id=0, has_side_effects=True, vmem_limit_bytes=48 * 1024 * 1024
        ),
    )(*(pltpu.with_memory_space_constraint(x, pltpu.HBM) for x in (imbalance, flow, potential, cost)))
    anywhere = pl.BlockSpec(memory_space=pl.ANY)
    flow_out, u_out, res = pl.pallas_call(
        finish,
        out_shape=(
            jax.ShapeDtypeStruct(flow.shape, f32),
            jax.ShapeDtypeStruct(potential.shape, f32),
            jax.ShapeDtypeStruct((1, pairs), f32),
        ),
        in_specs=[anywhere] * 3,
        out_specs=(hbm, hbm, hbm),
        scratch_shapes=[pltpu.VMEM(packed, f32), pltpu.VMEM((1, pairs), f32), pltpu.SemaphoreType.DMA((3,))],
    )(*(pltpu.with_memory_space_constraint(x, pltpu.VMEM) for x in (flow_out, u_out, res)))
    return flow_out, u_out, res.reshape(pairs)


def solution(mesh):
    placed = (P(None, "gy", "gx"), P(None, None, "gy", "gx"), P(None, "gy", "gx"), P("gy", "gx"))
    return jax.shard_map(
        functools.partial(local, mesh.shape["gy"], mesh.shape["gx"]),
        mesh=mesh,
        in_specs=placed,
        out_specs=(P(None, None, "gy", "gx"), P(None, "gy", "gx"), P()),
        check_vma=False,
    )
```

```python
import functools
import itertools

import jax
import jax.numpy as jnp
from jax import lax
from jax.experimental import pallas as pl
from jax.experimental.pallas import tpu as pltpu
from jax.sharding import PartitionSpec as P

ITERS = 12
LANES = 128
SUBS = 8

initial_step = 0.35
epsilon = 1e-06
MESH = pl.DeviceIdType.MESH


def kernel(
    ny, nx,
    imb_hbm, flow_hbm, u_hbm, cost_hbm,
    flow_hbm_out, u_hbm_out, res_out,
    imb_in, flow_in, u_in, cost_in,
    A, B, U, E, W, GA, GB, IM, CO,
    tau_ref, sig_ref,
    row_send, col_send, row_recv, col_recv, corner_recv, msg_send, msg_recv,
    ext_row, ext_col, ext_row_in, ext_col_in, cost_row, cost_col, cost_row_in, cost_col_in,
    grow, gcol, slope_row, slope_col,
    res_row, spare,
    halo_ssem, halo_rsem, msg_ssem, msg_rsem, out_sem, plane_sem,
):
    G, T, _, C = A.shape
    n = ny * nx
    rows = T * SUBS
    gy, gx = lax.axis_index("gy"), lax.axis_index("gx")
    me = gy * nx + gx
    up, down, left, right = gy > 0, gy < ny - 1, gx > 0, gx < nx - 1
    f32 = jnp.float32
    K = C // LANES

    def piece(ref, k):
        return ref.at[(slice(None),) * (len(ref.shape) - 1) + (pl.ds(k * LANES, LANES),)]

    def fetch_sem(i, g):
        return (out_sem.at[1], msg_ssem.at[g], halo_ssem.at[g], out_sem.at[0])[i]

    def start_fetch(i, g):
        for k in range(K):
            at = pl.ds(k * LANES, LANES)
            src, dst = (
                (cost_hbm.at[:, at], cost_in.at[k]), (u_hbm.at[g, :, at], u_in.at[k, g]),
                (flow_hbm.at[:, g, :, at], flow_in.at[k, :, g]), (imb_hbm.at[:, :, at], imb_in.at[k]),
            )[i]
            pltpu.make_async_copy(src, dst, fetch_sem(i, g)).start()

    def wait_fetch(i, g):
        whole = (cost_in, u_in.at[:, g], flow_in.at[:, :, g], imb_in)[i]
        pltpu.make_async_copy(whole, whole, fetch_sem(i, g)).wait()

    half = ny // 2
    low = gy < half
    xs = [lax.rem(gx + d, nx) for d in range(nx)]
    order = sorted(range(nx), key=lambda d: -min(d, nx - d))
    places = [(jnp.where(low, ny - 1 - j, j), xs[d]) for j in range(half) for d in order]
    high = jnp.where(low, ny - 1 - gy, gy) - half
    for k in range(1, ny - half):
        y = half + lax.rem(high + k, ny - half)
        places += [(jnp.where(low, ny - 1 - y, y), xs[d]) for d in order]
    places += [(gy, xs[d]) for d in order if d]

    start_fetch(1, 0)
    start_fetch(2, 0)
    start_fetch(0, 0)
    barrier = pltpu.get_barrier_semaphore()

    def greet(where):
        pl.semaphore_signal(barrier, inc=1, device_id=where, device_id_type=MESH)

    odd = lax.rem(gy, 2)
    column = [(lax.rem(gy + 2 * k, ny), gx) for k in range(1, half)]
    mates = [(gy, xs[d]) for d in order if d] + [(gy + 1 - 2 * odd, xs[d]) for d in order]
    low_side, high_side = odd == 1, odd == 0
    outside = [
        (jnp.logical_and(low_side, down), (gy + 1, gx)),
        (jnp.logical_and(low_side, jnp.logical_and(down, left)), (gy + 1, gx - 1)),
        (jnp.logical_and(high_side, up), (gy - 1, gx)),
        (jnp.logical_and(high_side, jnp.logical_and(up, right)), (gy - 1, gx + 1)),
    ]
    for where in column + mates:
        greet(where)
    guests = len(column) + len(mates)
    for ok, where in outside:
        guests = guests + jnp.where(ok, 1, 0)

        @pl.when(ok)
        def _(where=where):
            greet(where)

    def later(g, c):
        start_fetch(1, g)
        start_fetch(2, g)
        return c

    lax.fori_loop(1, G, later, 0)

    start_fetch(3, 0)

    def gather(ref, *index):
        at = pl.ds(index[-1], SUBS, stride=T)
        return jnp.concatenate([ref[(k,) + index[:-1] + (at, slice(None))] for k in range(K)], axis=1)

    def scatter(ref, value, *index):
        at = pl.ds(index[-1], SUBS, stride=T)
        for k in range(K):
            ref[(k,) + index[:-1] + (at, slice(None))] = value[:, k * LANES:(k + 1) * LANES]

    def line(ref, *index):
        return jnp.concatenate([ref[(k,) + index[:-1] + (pl.ds(index[-1], 1), slice(None))] for k in range(K)], axis=1)

    lane = lax.broadcasted_iota(jnp.int32, (SUBS, LANES), 1)
    sub = lax.broadcasted_iota(jnp.int32, (SUBS, LANES), 0)
    subw = lax.broadcasted_iota(jnp.int32, (SUBS, C), 0)
    ones = jnp.ones((SUBS, LANES), f32)

    def wide(x):
        return jnp.concatenate([x] * K, axis=1)

    def row8(x):
        return jnp.broadcast_to(x, (SUBS, x.shape[1]))

    def turn_lanes(x, by):
        return pltpu.roll(x, by % LANES, 1) if by % LANES else x

    def to_left(x, entering):
        r = pltpu.roll(x, C - 1, 1)
        lanes = lax.broadcasted_iota(jnp.int32, entering.shape, 1)
        tail = jnp.where(lanes == LANES - 1, entering, r[:, C - LANES:])
        return jnp.concatenate([r[:, : C - LANES], tail], axis=1)

    def to_right(x, entering):
        r = pltpu.roll(x, 1, 1)
        head = jnp.where(lane == 0, entering, r[:, :LANES])
        return jnp.concatenate([head, r[:, LANES:]], axis=1)

    def pack_first(acc, v, t):
        return jnp.where(lane == t, turn_lanes(v, t), acc)

    def pack_last(acc, v, t):
        return jnp.where(lane == t, turn_lanes(v, t + 1), acc)

    def remote(src, dst, ssem, rsem, where):
        return pltpu.make_async_remote_copy(
            src_ref=src, dst_ref=dst, send_sem=ssem, recv_sem=rsem, device_id=where, device_id_type=MESH
        )

    def halos(slot, g):
        sems = (halo_ssem.at[g], halo_rsem.at[slot, g])
        head, tail = row_send.at[slot, 0, g], row_send.at[slot, 1, g]
        return [
            (jnp.logical_and(down, left), remote(tail.at[:, pl.ds(0, LANES)], corner_recv.at[slot, 0, g], *sems, (gy + 1, gx - 1))),
            (jnp.logical_and(up, right), remote(head.at[:, pl.ds(C - LANES, LANES)], corner_recv.at[slot, 1, g], *sems, (gy - 1, gx + 1))),
            (up, remote(head, row_recv.at[slot, 0, g], *sems, (gy - 1, gx))),
            (down, remote(tail, row_recv.at[slot, 1, g], *sems, (gy + 1, gx))),
            (left, remote(col_send.at[slot, 0, g], col_recv.at[slot, 0, g], *sems, (gy, gx - 1))),
            (right, remote(col_send.at[slot, 1, g], col_recv.at[slot, 1, g], *sems, (gy, gx + 1))),
        ]

    def extras(g):
        sems = (msg_ssem.at[g], msg_rsem.at[0, g])
        return [
            (down, remote(ext_row.at[g], ext_row_in.at[g], *sems, (gy + 1, gx))),
            (right, remote(ext_col.at[g], ext_col_in.at[g], *sems, (gy, gx + 1))),
        ]

    def prices():
        sems = (out_sem.at[1], out_sem.at[2])
        return [
            (down, remote(cost_row, cost_row_in, *sems, (gy + 1, gx))),
            (right, remote(cost_col, cost_col_in, *sems, (gy, gx + 1))),
        ]

    def start_all(copies):
        for ok, copy in copies:
            @pl.when(ok)
            def _(copy=copy):
                copy.start()

    sides = [c for c in itertools.product((0, 1), repeat=4) if (c[0] or c[1]) and (c[2] or c[3])]

    def lies(case):
        flags = [f if has else jnp.logical_not(f) for f, has in zip((up, down, left, right), case)]
        return functools.reduce(jnp.logical_and, flags)

    def wait_rows(sem, count):
        totals_of = {}
        for case in sides:
            totals_of.setdefault(count(*case), []).append(case)
        for total, cases in totals_of.items():
            if total:
                @pl.when(functools.reduce(jnp.logical_or, [lies(case) for case in cases]))
                def _(total=total):
                    whole = spare.at[pl.ds(0, total)]
                    pltpu.make_async_copy(whole, whole, sem).wait()

    def wait_halos(slot, g):
        count = lambda u, d, l, r: K * (u + d) + SUBS * (l + r) + u * r + d * l
        wait_rows(halo_rsem.at[slot, g], count)
        wait_rows(halo_ssem.at[g], count)

    def wait_edges(ssem, rsem, parts):
        wait_rows(rsem, lambda u, d, l, r: parts * (K * u + SUBS * l))
        wait_rows(ssem, lambda u, d, l, r: parts * (K * d + SUBS * r))

    def send_message(slot, g, rows):
        for k, row in enumerate(rows):
            msg_send[slot, g, k:k + 1] = row
            msg_recv[slot, g, me, k:k + 1] = row
        for where in places:
            remote(
                msg_send.at[slot, g], msg_recv.at[slot, g, me], msg_ssem.at[g], msg_rsem.at[slot, g], where
            ).start()

    def wait_message(slot, g):
        whole = msg_recv.at[slot, g, pl.ds(0, n - 1)]
        pltpu.make_async_copy(whole, whole, msg_rsem.at[slot, g]).wait()
        pltpu.make_async_copy(whole, whole, msg_ssem.at[g]).wait()

    def totals(slot, g):
        parts = [msg_recv[slot, g, k] for k in range(n)]
        while len(parts) > 1:
            parts = [sum(parts[k + 1:k + 2], parts[k]) for k in range(0, len(parts), 2)]
        return [jnp.sum(row8(parts[0][k:k + 1]), axis=1, keepdims=True) for k in range(2)]

    def fold(x, y):
        x, y = (sum((v[:, k * LANES:(k + 1) * LANES] for k in range(1, K)), v[:, :LANES]) for v in (x, y))
        half = SUBS // 2
        z = jnp.where(sub < half, x + pltpu.roll(x, half, 0), y + pltpu.roll(y, half, 0))
        z = z + pltpu.roll(z, 1, 0)
        z = z + pltpu.roll(z, 2, 0)
        return z[half - 1:half], z[SUBS - 1:]


    def edges(g, c):
        wait_fetch(1, g)
        packs = [ones] * 4
        row_send[0, 0, g] = line(u_in, g, 0)
        row_send[0, 1, g] = line(u_in, g, rows - 1)
        for t in range(T):
            at = pl.ds(t, SUBS, stride=T)
            packs[0] = pack_first(packs[0], u_in[0, g, at, :], t)
            packs[1] = pack_last(packs[1], u_in[K - 1, g, at, :], t)
        wait_fetch(2, g)
        for t in range(T):
            at = pl.ds(t, SUBS, stride=T)
            packs[2] = pack_last(packs[2], flow_in[K - 1, 0, g, at, :], t)
            packs[3] = pack_last(packs[3], flow_in[K - 1, 1, g, at, :], t)
        col_send[0, 0, g] = packs[0]
        col_send[0, 1, g] = packs[1]
        for k in range(2):
            ext_col[g, k] = packs[2 + k]
            ext_row[g, k] = line(flow_in, k, g, rows - 1)
        return c

    for missing, refs in (
        (jnp.logical_not(down), [row_recv.at[s, 0] for s in range(2)]),
        (jnp.logical_not(up), [row_recv.at[s, 1] for s in range(2)] + [ext_row_in]),
        (jnp.logical_not(right), [col_recv.at[s, 0] for s in range(2)]),
        (jnp.logical_not(left), [col_recv.at[s, 1] for s in range(2)] + [ext_col_in]),
        (jnp.logical_not(jnp.logical_and(up, right)), [corner_recv.at[s, 0] for s in range(2)]),
        (jnp.logical_not(jnp.logical_and(down, left)), [corner_recv.at[s, 1] for s in range(2)]),
    ):
        @pl.when(missing)
        def _(refs=refs):
            for ref in refs:
                ref[...] = jnp.zeros(ref.shape, f32)

    for missing, ref in ((jnp.logical_not(up), cost_row_in), (jnp.logical_not(left), cost_col_in)):
        @pl.when(missing)
        def _(ref=ref):
            ref[...] = jnp.ones(ref.shape, f32)

    edges(0, 0)
    pl.semaphore_wait(barrier, guests)
    for where in column:
        pl.semaphore_signal(plane_sem, inc=1, device_id=where, device_id_type=MESH)
    start_all(halos(0, 0) + extras(0))
    wait_fetch(0, 0)
    pack = ones
    for t in range(T):
        CO[t] = gather(cost_in, t)
        pack = pack_last(pack, CO[t][:, C - LANES:], t)
    cost_col[...] = pack
    cost_row[...] = line(cost_in, rows - 1)
    start_all(prices())

    def announce(g, c):
        edges(g, c)
        start_all(halos(0, g) + extras(g))
        return c

    lax.fori_loop(1, G, announce, 0)

    no_lane = jnp.zeros((SUBS, LANES), f32)

    def above_first(a_last, ghost):
        return jnp.where(subw == 0, row8(ghost), pltpu.roll(a_last, 1, 0))

    def below_last(u_first):
        return jnp.where(subw == SUBS - 1, 0.0, pltpu.roll(u_first, SUBS - 1, 0))

    wait_fetch(3, 0)

    def load(g, c):
        for t in range(T):
            A[g, t] = gather(flow_in, 0, g, t)
            B[g, t] = gather(flow_in, 1, g, t)
            U[g, t] = gather(u_in, g, t)
            IM[g, t] = gather(imb_in, g, t)
        for t in range(T):
            a, b, u = A[g, t], B[g, t], U[g, t]
            above = A[g, t - 1] if t else above_first(A[g, T - 1], jnp.zeros((1, C), f32))
            E[g, t] = ((a - above) + (b - to_right(b, no_lane))) + IM[g, t]
            GA[g, t] = (U[g, t + 1] if t < T - 1 else below_last(U[g, 0])) - u
            GB[g, t] = to_left(u, no_lane) - u
        return c

    lax.fori_loop(0, G, load, 0)
    pl.semaphore_wait(plane_sem, len(column))

    def divergence(t, a, above, b, gb):
        return ((a - above) + (b - to_right(b, turn_lanes(gb, -t))))

    def begin(g):
        wait_edges(msg_ssem.at[g], msg_rsem.at[0, g], 2)
        for k in range(2):
            grow[g, k] = ext_row_in[g, k]
            gcol[g, k] = ext_col_in[g, k]
        gb = gcol[g, 1]
        E[g, 0] = E[g, 0] - jnp.where(subw == 0, row8(grow[g, 0]), 0.0)
        for t in range(T):
            E[g, t, :, :LANES] = E[g, t, :, :LANES] - jnp.where(lane == 0, turn_lanes(gb, -t), 0.0)

    def slopes(slot, g):
        wait_halos(slot, g)
        u = row_recv[slot, 1, g]
        u_right = to_left(u, turn_lanes(corner_recv[slot, 0, g], LANES - 1))
        zero = jnp.zeros_like(u)
        slope_row[g, 0] = jnp.where(up, row_send[slot, 0, g] - u, zero)
        slope_row[g, 1] = jnp.where(up, u_right - u, zero)
        u = col_recv[slot, 1, g]
        turn = turn_lanes(pltpu.roll(u, SUBS - 1, 0), T - 1)
        turn = jnp.where(sub == SUBS - 1, row8(turn_lanes(corner_recv[slot, 1, g], T)), turn)
        u_down = jnp.where(lane == T - 1, turn, turn_lanes(u, -1))
        zero = jnp.zeros_like(u)
        slope_col[g, 0] = jnp.where(left, u_down - u, zero)
        slope_col[g, 1] = jnp.where(left, col_send[slot, 0, g] - u, zero)
        GA[g, T - 1] = GA[g, T - 1] + jnp.where(subw == SUBS - 1, row8(row_recv[slot, 0, g]), 0.0)
        beside = col_recv[slot, 0, g]
        for t in range(T):
            entering = jnp.where(lane == LANES - 1, turn_lanes(beside, LANES - 1 - t), 0.0)
            GB[g, t, :, C - LANES:] = GB[g, t, :, C - LANES:] + entering

    def shrink(va, vb, t):
        f = jnp.maximum(1.0 - t * lax.rsqrt(va * va + vb * vb), 0.0)
        return f * va, f * vb

    def adapt(slot, g):
        wait_message(slot, g)
        sigma = sig_ref[g]
        primal, dual = (jnp.broadcast_to(v, (SUBS, LANES)) for v in totals(slot, g))
        primal = primal + epsilon
        dual = sigma * sigma * dual + epsilon
        root = lax.rsqrt(primal) * (dual * lax.rsqrt(dual))
        s = lax.rsqrt(root)
        tau = tau_ref[g] * (root * s)
        sigma = sigma * s
        tau_ref[g] = tau
        sig_ref[g] = sigma
        return tau, sigma

    def sweep(g, other, tau, closing):
        wtau = wide(tau)
        tau1 = wtau[0:1]
        ghost_a, ghost_b = shrink(
            grow[g, 0] + tau1 * slope_row[g, 0], grow[g, 1] + tau1 * slope_row[g, 1], tau1 * cost_row_in[...]
        )
        side_a, side_b = shrink(
            gcol[g, 0] + tau * slope_col[g, 0], gcol[g, 1] + tau * slope_col[g, 1], tau * cost_col_in[...]
        )
        grow[g, 0] = ghost_a
        grow[g, 1] = ghost_b
        gcol[g, 0] = side_a
        gcol[g, 1] = side_b
        acc_p = jnp.zeros((SUBS, C), f32)
        acc_d = jnp.zeros((SUBS, C), f32)

        def dual(t, a2, above, b2):
            nonlocal acc_d
            q2 = divergence(t, a2, above, b2, side_b)
            w = (q2 + q2) - E[g, t]
            W[g, t] = w
            if closing:
                w = q2 - IM[g, t]
            acc_d = acc_d + w * w

        for t in range(T):
            a, b = A[g, t], B[g, t]
            a2, b2 = shrink(a + wtau * GA[g, t], b + wtau * GB[g, t], wtau * CO[t])
            A[g, t] = a2
            B[g, t] = b2
            if not closing:
                da, db = a2 - a, b2 - b
                acc_p = acc_p + (da * da + db * db)
            if t:
                dual(t, a2, above, b2)
            else:
                a_first, b_first = a2, b2
            above = a2
        dual(0, a_first, above_first(above, ghost_a), b_first)
        send_message(other, g, fold(acc_p, acc_d))

    ends = sorted({0, K - 1})

    def chunk(k):
        return pl.ds(k * LANES, LANES)

    def depart(other, g, sigma):
        packs = [ones, ones]
        for t in range(T):
            for k in range(K) if t in (0, T - 1) else ends:
                u2 = U[g, t, :, chunk(k)] + sigma * W[g, t, :, chunk(k)]
                U[g, t, :, chunk(k)] = u2
                if k == 0:
                    packs[0] = pack_first(packs[0], u2, t)
                if k == K - 1:
                    packs[1] = pack_last(packs[1], u2, t)
                if t == 0:
                    row_send[other, 0, g, :, chunk(k)] = u2[0:1]
                if t == T - 1:
                    row_send[other, 1, g, :, chunk(k)] = u2[SUBS - 1:]
        for k in range(2):
            col_send[other, k, g] = packs[k]
        start_all(halos(other, g))

    def settle(g, c):
        sigma = sig_ref[g]
        first = prev = U[g, 0]
        for t in range(T):
            w = W[g, t]
            E[g, t] = 0.5 * (w + E[g, t]) + IM[g, t]
            if t in (0, T - 1):
                u2 = U[g, t]
            else:
                inner = [
                    U[g, t, :, chunk(k)] if k in ends else U[g, t, :, chunk(k)] + sigma * w[:, k * LANES:(k + 1) * LANES]
                    for k in range(K)
                ]
                for k in range(K):
                    if k not in ends:
                        U[g, t, :, chunk(k)] = inner[k]
                u2 = jnp.concatenate(inner, axis=1)
            GB[g, t] = to_left(u2, no_lane) - u2
            if t:
                GA[g, t - 1] = u2 - prev
            if t == T - 1:
                GA[g, t] = below_last(first) - u2
            prev = u2
        return c

    def opening(g, c):
        begin(g)
        slopes(0, g)
        step = jnp.full((SUBS, LANES), initial_step, f32)
        tau_ref[g] = step
        sig_ref[g] = step
        @pl.when(g == 0)
        def _():
            wait_edges(out_sem.at[1], out_sem.at[2], 1)

        sweep(g, 1, step, False)
        depart(1, g, step)
        return c

    lax.fori_loop(0, G, opening, 0)
    lax.fori_loop(0, G, settle, 0)
    slopes(1, 0)

    def turn(i, c):
        slot = lax.rem(i, 2)
        other = 1 - slot

        def one(g, c):
            tau, sigma = adapt(slot, g)
            sweep(g, other, tau, False)
            depart(other, g, sigma)

            @pl.when(g < G - 1)
            def _():
                slopes(slot, g + 1)

            return c

        lax.fori_loop(0, G, one, c)
        lax.fori_loop(0, G, settle, c)
        slopes(other, 0)
        return c

    lax.fori_loop(1, ITERS - 1, turn, 0)
    slot = (ITERS - 1) % 2

    def close(g, c):
        sweep(g, 1 - slot, adapt(slot, g)[0], True)

        @pl.when(g < G - 1)
        def _():
            slopes(slot, g + 1)

        return c

    def unload(g, c):
        wsigma = wide(sig_ref[g])
        for t in range(T):
            scatter(flow_in, A[g, t], 0, g, t)
            scatter(flow_in, B[g, t], 1, g, t)
            scatter(u_in, U[g, t] + wsigma * W[g, t], g, t)
        return c

    lax.fori_loop(0, G, close, 0)
    lax.fori_loop(0, G, unload, 0)
    results = [
        pltpu.make_async_copy(src.at[k], piece(dst, k), out_sem.at[i])
        for i, (src, dst) in enumerate(((flow_in, flow_hbm_out), (u_in, u_hbm_out)))
        for k in range(K)
    ]
    for copy in results:
        copy.start()
    cells = T * SUBS * C * n
    row = ones
    for g in range(G):
        wait_message(1 - slot, g)
        row = jnp.where(lane == g, totals(1 - slot, g)[1] / cells, row)
    res_row[...] = row
    give = pltpu.make_async_copy(res_row, res_out, out_sem.at[2])
    give.start()
    for i, whole in enumerate((flow_hbm_out, u_hbm_out)):
        pltpu.make_async_copy(whole, whole, out_sem.at[i]).wait()
    give.wait()


def finish(flow_in, u_in, res_in, flow_out, u_out, res_out, row, short, sems):
    pick = pltpu.make_async_copy(res_in, row, sems.at[0])
    pick.start()
    copies = [pltpu.make_async_copy(u_in, u_out, sems.at[1]), pltpu.make_async_copy(flow_in, flow_out, sems.at[2])]
    for copy in copies:
        copy.start()
    pick.wait()
    short[...] = row[0:1, 0:short.shape[1]]
    give = pltpu.make_async_copy(short, res_out, sems.at[0])
    give.start()
    for copy in copies:
        copy.wait()
    give.wait()


def local(ny, nx, imbalance, flow, potential, cost):
    pairs, rows, cols = imbalance.shape
    T = rows // SUBS
    n = ny * nx
    assert rows % SUBS == 0 and cols % LANES == 0 and 4 <= T < LANES and ny % 2 == 0 and nx > 1
    assert pairs <= LANES
    G = pairs
    f32 = jnp.float32
    block = (pairs, T, SUBS, cols)
    packed = (SUBS, LANES)
    K = cols // LANES
    hbm = pl.BlockSpec(memory_space=pltpu.HBM)
    flow_out, u_out, res = pl.pallas_call(
        functools.partial(kernel, ny, nx),
        out_shape=(
            jax.ShapeDtypeStruct(flow.shape, f32),
            jax.ShapeDtypeStruct(potential.shape, f32),
            jax.ShapeDtypeStruct(packed, f32),
        ),
        in_specs=[hbm] * 4,
        out_specs=(hbm, hbm, hbm),
        scratch_shapes=[
            pltpu.VMEM((K, pairs, rows, LANES), f32), pltpu.VMEM((K, 2, pairs, rows, LANES), f32),
            pltpu.VMEM((K, pairs, rows, LANES), f32), pltpu.VMEM((K, rows, LANES), f32),
        ] + [pltpu.VMEM(block, f32)] * 8 + [
            pltpu.VMEM(block[1:], f32),
            pltpu.VMEM((G,) + packed, f32), pltpu.VMEM((G,) + packed, f32),
            pltpu.VMEM((2, 2, G, 1, cols), f32), pltpu.VMEM((2, 2, G) + packed, f32),
            pltpu.VMEM((2, 2, G, 1, cols), f32), pltpu.VMEM((2, 2, G) + packed, f32),
            pltpu.VMEM((2, 2, G, 1, LANES), f32),
            pltpu.VMEM((2, G, 2, LANES), f32), pltpu.VMEM((2, G, n, 2, LANES), f32),
            pltpu.VMEM((G, 2, 1, cols), f32), pltpu.VMEM((G, 2) + packed, f32),
            pltpu.VMEM((G, 2, 1, cols), f32), pltpu.VMEM((G, 2) + packed, f32),
            pltpu.VMEM((1, cols), f32), pltpu.VMEM(packed, f32),
            pltpu.VMEM((1, cols), f32), pltpu.VMEM(packed, f32),
            pltpu.VMEM((G, 2, 1, cols), f32), pltpu.VMEM((G, 2) + packed, f32),
            pltpu.VMEM((G, 2, 1, cols), f32), pltpu.VMEM((G, 2) + packed, f32),
            pltpu.VMEM(packed, f32), pltpu.VMEM((2 * K + 2 * SUBS + 2, 1, LANES), f32),
            pltpu.SemaphoreType.DMA((G,)), pltpu.SemaphoreType.DMA((2, G)),
            pltpu.SemaphoreType.DMA((G,)), pltpu.SemaphoreType.DMA((2, G)),
            pltpu.SemaphoreType.DMA((3,)), pltpu.SemaphoreType.REGULAR,
        ],
        compiler_params=pltpu.CompilerParams(
            collective_id=0, has_side_effects=True, vmem_limit_bytes=48 * 1024 * 1024
        ),
    )(*(pltpu.with_memory_space_constraint(x, pltpu.HBM) for x in (imbalance, flow, potential, cost)))
    anywhere = pl.BlockSpec(memory_space=pl.ANY)
    flow_out, u_out, res = pl.pallas_call(
        finish,
        out_shape=(
            jax.ShapeDtypeStruct(flow.shape, f32),
            jax.ShapeDtypeStruct(potential.shape, f32),
            jax.ShapeDtypeStruct((1, pairs), f32),
        ),
        in_specs=[anywhere] * 3,
        out_specs=(hbm, hbm, hbm),
        scratch_shapes=[pltpu.VMEM(packed, f32), pltpu.VMEM((1, pairs), f32), pltpu.SemaphoreType.DMA((3,))],
    )(*(pltpu.with_memory_space_constraint(x, pltpu.VMEM) for x in (flow_out, u_out, res)))
    return flow_out, u_out, res.reshape(pairs)


def solution(mesh):
    placed = (P(None, "gy", "gx"), P(None, None, "gy", "gx"), P(None, "gy", "gx"), P("gy", "gx"))
    return jax.shard_map(
        functools.partial(local, mesh.shape["gy"], mesh.shape["gx"]),
        mesh=mesh,
        in_specs=placed,
        out_specs=(P(None, None, "gy", "gx"), P(None, "gy", "gx"), P()),
        check_vma=False,
    )
```

```python
import functools
import itertools

import jax
import jax.numpy as jnp
from jax import lax
from jax.experimental import pallas as pl
from jax.experimental.pallas import tpu as pltpu
from jax.sharding import PartitionSpec as P

ITERS = 12
LANES = 128
SUBS = 8

initial_step = 0.35
epsilon = 1e-06
MESH = pl.DeviceIdType.MESH


def kernel(
    ny, nx,
    imb_hbm, flow_hbm, u_hbm, cost_hbm,
    flow_hbm_out, u_hbm_out, res_out,
    imb_in, flow_in, u_in, cost_in,
    A, B, U, E, W, GA, GB, IM, CO,
    tau_ref, sig_ref,
    row_send, col_send, row_recv, col_recv, corner_recv, msg_send, msg_recv,
    ext_row, ext_col, ext_row_in, ext_col_in, cost_row, cost_col, cost_row_in, cost_col_in,
    grow, gcol, slope_row, slope_col,
    res_row, spare,
    halo_ssem, halo_rsem, msg_ssem, msg_rsem, out_sem, plane_sem,
):
    G, T, _, C = A.shape
    n = ny * nx
    rows = T * SUBS
    gy, gx = lax.axis_index("gy"), lax.axis_index("gx")
    me = gy * nx + gx
    up, down, left, right = gy > 0, gy < ny - 1, gx > 0, gx < nx - 1
    f32 = jnp.float32
    K = C // LANES

    def piece(ref, k):
        return ref.at[(slice(None),) * (len(ref.shape) - 1) + (pl.ds(k * LANES, LANES),)]

    def fetch_sem(i, g):
        return (out_sem.at[1], msg_ssem.at[g], halo_ssem.at[g], out_sem.at[0])[i]

    def start_fetch(i, g):
        for k in range(K):
            at = pl.ds(k * LANES, LANES)
            src, dst = (
                (cost_hbm.at[:, at], cost_in.at[k]), (u_hbm.at[g, :, at], u_in.at[k, g]),
                (flow_hbm.at[:, g, :, at], flow_in.at[k, :, g]), (imb_hbm.at[:, :, at], imb_in.at[k]),
            )[i]
            pltpu.make_async_copy(src, dst, fetch_sem(i, g)).start()

    def wait_fetch(i, g):
        whole = (cost_in, u_in.at[:, g], flow_in.at[:, :, g], imb_in)[i]
        pltpu.make_async_copy(whole, whole, fetch_sem(i, g)).wait()

    half = ny // 2
    low = gy < half
    xs = [lax.rem(gx + d, nx) for d in range(nx)]
    order = sorted(range(nx), key=lambda d: -min(d, nx - d))
    high = jnp.where(low, ny - 1 - gy, gy) - half
    across = [half + lax.rem(high + half - j, half) for j in range(half)]
    places = [(jnp.where(low, y, ny - 1 - y), xs[d]) for y in across for d in order]
    for k in range(1, ny - half):
        y = half + lax.rem(high + k, ny - half)
        places += [(jnp.where(low, ny - 1 - y, y), xs[d]) for d in order]
    places += [(gy, xs[d]) for d in order if d]

    start_fetch(1, 0)
    start_fetch(2, 0)
    start_fetch(0, 0)
    barrier = pltpu.get_barrier_semaphore()

    def greet(where):
        pl.semaphore_signal(barrier, inc=1, device_id=where, device_id_type=MESH)

    odd = lax.rem(gy, 2)
    column = [(lax.rem(gy + 2 * k, ny), gx) for k in range(1, half)]
    mates = [(gy, xs[d]) for d in order if d] + [(gy + 1 - 2 * odd, xs[d]) for d in order]
    low_side, high_side = odd == 1, odd == 0
    outside = [
        (jnp.logical_and(low_side, down), (gy + 1, gx)),
        (jnp.logical_and(low_side, jnp.logical_and(down, left)), (gy + 1, gx - 1)),
        (jnp.logical_and(high_side, up), (gy - 1, gx)),
        (jnp.logical_and(high_side, jnp.logical_and(up, right)), (gy - 1, gx + 1)),
    ]
    for where in column + mates:
        greet(where)
    guests = len(column) + len(mates)
    for ok, where in outside:
        guests = guests + jnp.where(ok, 1, 0)

        @pl.when(ok)
        def _(where=where):
            greet(where)

    def later(g, c):
        start_fetch(1, g)
        start_fetch(2, g)
        return c

    lax.fori_loop(1, G, later, 0)

    start_fetch(3, 0)

    def gather(ref, *index):
        at = pl.ds(index[-1], SUBS, stride=T)
        return jnp.concatenate([ref[(k,) + index[:-1] + (at, slice(None))] for k in range(K)], axis=1)

    def scatter(ref, value, *index):
        at = pl.ds(index[-1], SUBS, stride=T)
        for k in range(K):
            ref[(k,) + index[:-1] + (at, slice(None))] = value[:, k * LANES:(k + 1) * LANES]

    def line(ref, *index):
        return jnp.concatenate([ref[(k,) + index[:-1] + (pl.ds(index[-1], 1), slice(None))] for k in range(K)], axis=1)

    lane = lax.broadcasted_iota(jnp.int32, (SUBS, LANES), 1)
    sub = lax.broadcasted_iota(jnp.int32, (SUBS, LANES), 0)
    subw = lax.broadcasted_iota(jnp.int32, (SUBS, C), 0)
    ones = jnp.ones((SUBS, LANES), f32)

    def wide(x):
        return jnp.concatenate([x] * K, axis=1)

    def row8(x):
        return jnp.broadcast_to(x, (SUBS, x.shape[1]))

    def turn_lanes(x, by):
        return pltpu.roll(x, by % LANES, 1) if by % LANES else x

    def to_left(x, entering):
        r = pltpu.roll(x, C - 1, 1)
        lanes = lax.broadcasted_iota(jnp.int32, entering.shape, 1)
        tail = jnp.where(lanes == LANES - 1, entering, r[:, C - LANES:])
        return jnp.concatenate([r[:, : C - LANES], tail], axis=1)

    def to_right(x, entering):
        r = pltpu.roll(x, 1, 1)
        head = jnp.where(lane == 0, entering, r[:, :LANES])
        return jnp.concatenate([head, r[:, LANES:]], axis=1)

    def pack_first(acc, v, t):
        return jnp.where(lane == t, turn_lanes(v, t), acc)

    def pack_last(acc, v, t):
        return jnp.where(lane == t, turn_lanes(v, t + 1), acc)

    def remote(src, dst, ssem, rsem, where):
        return pltpu.make_async_remote_copy(
            src_ref=src, dst_ref=dst, send_sem=ssem, recv_sem=rsem, device_id=where, device_id_type=MESH
        )

    def halos(slot, g):
        sems = (halo_ssem.at[g], halo_rsem.at[slot, g])
        head, tail = row_send.at[slot, 0, g], row_send.at[slot, 1, g]
        return [
            (jnp.logical_and(down, left), remote(tail.at[:, pl.ds(0, LANES)], corner_recv.at[slot, 0, g], *sems, (gy + 1, gx - 1))),
            (jnp.logical_and(up, right), remote(head.at[:, pl.ds(C - LANES, LANES)], corner_recv.at[slot, 1, g], *sems, (gy - 1, gx + 1))),
            (up, remote(head, row_recv.at[slot, 0, g], *sems, (gy - 1, gx))),
            (down, remote(tail, row_recv.at[slot, 1, g], *sems, (gy + 1, gx))),
            (left, remote(col_send.at[slot, 0, g], col_recv.at[slot, 0, g], *sems, (gy, gx - 1))),
            (right, remote(col_send.at[slot, 1, g], col_recv.at[slot, 1, g], *sems, (gy, gx + 1))),
        ]

    def extras(g):
        sems = (msg_ssem.at[g], msg_rsem.at[0, g])
        return [
            (down, remote(ext_row.at[g], ext_row_in.at[g], *sems, (gy + 1, gx))),
            (right, remote(ext_col.at[g], ext_col_in.at[g], *sems, (gy, gx + 1))),
        ]

    def prices():
        sems = (out_sem.at[1], out_sem.at[2])
        return [
            (down, remote(cost_row, cost_row_in, *sems, (gy + 1, gx))),
            (right, remote(cost_col, cost_col_in, *sems, (gy, gx + 1))),
        ]

    def start_all(copies):
        for ok, copy in copies:
            @pl.when(ok)
            def _(copy=copy):
                copy.start()

    sides = [c for c in itertools.product((0, 1), repeat=4) if (c[0] or c[1]) and (c[2] or c[3])]

    def lies(case):
        flags = [f if has else jnp.logical_not(f) for f, has in zip((up, down, left, right), case)]
        return functools.reduce(jnp.logical_and, flags)

    def wait_rows(sem, count):
        totals_of = {}
        for case in sides:
            totals_of.setdefault(count(*case), []).append(case)
        for total, cases in totals_of.items():
            if total:
                @pl.when(functools.reduce(jnp.logical_or, [lies(case) for case in cases]))
                def _(total=total):
                    whole = spare.at[pl.ds(0, total)]
                    pltpu.make_async_copy(whole, whole, sem).wait()

    def wait_halos(slot, g):
        count = lambda u, d, l, r: K * (u + d) + SUBS * (l + r) + u * r + d * l
        wait_rows(halo_rsem.at[slot, g], count)
        wait_rows(halo_ssem.at[g], count)

    def wait_edges(ssem, rsem, parts):
        wait_rows(rsem, lambda u, d, l, r: parts * (K * u + SUBS * l))
        wait_rows(ssem, lambda u, d, l, r: parts * (K * d + SUBS * r))

    def send_message(slot, g, rows):
        for k, row in enumerate(rows):
            msg_send[slot, g, k:k + 1] = row
            msg_recv[slot, g, me, k:k + 1] = row
        for where in places:
            remote(
                msg_send.at[slot, g], msg_recv.at[slot, g, me], msg_ssem.at[g], msg_rsem.at[slot, g], where
            ).start()

    def wait_message(slot, g):
        whole = msg_recv.at[slot, g, pl.ds(0, n - 1)]
        pltpu.make_async_copy(whole, whole, msg_rsem.at[slot, g]).wait()
        pltpu.make_async_copy(whole, whole, msg_ssem.at[g]).wait()

    def totals(slot, g):
        parts = [msg_recv[slot, g, k] for k in range(n)]
        while len(parts) > 1:
            parts = [sum(parts[k + 1:k + 2], parts[k]) for k in range(0, len(parts), 2)]
        return [jnp.sum(row8(parts[0][k:k + 1]), axis=1, keepdims=True) for k in range(2)]

    def fold(x, y):
        x, y = (sum((v[:, k * LANES:(k + 1) * LANES] for k in range(1, K)), v[:, :LANES]) for v in (x, y))
        half = SUBS // 2
        z = jnp.where(sub < half, x + pltpu.roll(x, half, 0), y + pltpu.roll(y, half, 0))
        z = z + pltpu.roll(z, 1, 0)
        z = z + pltpu.roll(z, 2, 0)
        return z[half - 1:half], z[SUBS - 1:]


    def edges(g, c):
        wait_fetch(1, g)
        packs = [ones] * 4
        row_send[0, 0, g] = line(u_in, g, 0)
        row_send[0, 1, g] = line(u_in, g, rows - 1)
        for t in range(T):
            at = pl.ds(t, SUBS, stride=T)
            packs[0] = pack_first(packs[0], u_in[0, g, at, :], t)
            packs[1] = pack_last(packs[1], u_in[K - 1, g, at, :], t)
        wait_fetch(2, g)
        for t in range(T):
            at = pl.ds(t, SUBS, stride=T)
            packs[2] = pack_last(packs[2], flow_in[K - 1, 0, g, at, :], t)
            packs[3] = pack_last(packs[3], flow_in[K - 1, 1, g, at, :], t)
        col_send[0, 0, g] = packs[0]
        col_send[0, 1, g] = packs[1]
        for k in range(2):
            ext_col[g, k] = packs[2 + k]
            ext_row[g, k] = line(flow_in, k, g, rows - 1)
        return c

    for missing, refs in (
        (jnp.logical_not(down), [row_recv.at[s, 0] for s in range(2)]),
        (jnp.logical_not(up), [row_recv.at[s, 1] for s in range(2)] + [ext_row_in]),
        (jnp.logical_not(right), [col_recv.at[s, 0] for s in range(2)]),
        (jnp.logical_not(left), [col_recv.at[s, 1] for s in range(2)] + [ext_col_in]),
        (jnp.logical_not(jnp.logical_and(up, right)), [corner_recv.at[s, 0] for s in range(2)]),
        (jnp.logical_not(jnp.logical_and(down, left)), [corner_recv.at[s, 1] for s in range(2)]),
    ):
        @pl.when(missing)
        def _(refs=refs):
            for ref in refs:
                ref[...] = jnp.zeros(ref.shape, f32)

    for missing, ref in ((jnp.logical_not(up), cost_row_in), (jnp.logical_not(left), cost_col_in)):
        @pl.when(missing)
        def _(ref=ref):
            ref[...] = jnp.ones(ref.shape, f32)

    edges(0, 0)
    pl.semaphore_wait(barrier, guests)
    for where in column:
        pl.semaphore_signal(plane_sem, inc=1, device_id=where, device_id_type=MESH)
    start_all(halos(0, 0) + extras(0))
    wait_fetch(0, 0)
    pack = ones
    for t in range(T):
        CO[t] = gather(cost_in, t)
        pack = pack_last(pack, CO[t][:, C - LANES:], t)
    cost_col[...] = pack
    cost_row[...] = line(cost_in, rows - 1)
    start_all(prices())

    def announce(g, c):
        edges(g, c)
        start_all(halos(0, g) + extras(g))
        return c

    lax.fori_loop(1, G, announce, 0)

    no_lane = jnp.zeros((SUBS, LANES), f32)

    def above_first(a_last, ghost):
        return jnp.where(subw == 0, ghost, pltpu.roll(a_last, 1, 0))

    def below_last(u_first):
        return jnp.where(subw == SUBS - 1, 0.0, pltpu.roll(u_first, SUBS - 1, 0))

    wait_fetch(3, 0)

    def load(g, c):
        for t in range(T):
            A[g, t] = gather(flow_in, 0, g, t)
            B[g, t] = gather(flow_in, 1, g, t)
            U[g, t] = gather(u_in, g, t)
            IM[g, t] = gather(imb_in, g, t)
        for t in range(T):
            a, b, u = A[g, t], B[g, t], U[g, t]
            above = A[g, t - 1] if t else above_first(A[g, T - 1], 0.0)
            E[g, t] = ((a - above) + (b - to_right(b, no_lane))) + IM[g, t]
            GA[g, t] = (U[g, t + 1] if t < T - 1 else below_last(U[g, 0])) - u
            GB[g, t] = to_left(u, no_lane) - u
        return c

    lax.fori_loop(0, G, load, 0)
    pl.semaphore_wait(plane_sem, len(column))

    def divergence(t, a, above, b, gb):
        return ((a - above) + (b - to_right(b, turn_lanes(gb, -t))))

    def begin(g):
        wait_edges(msg_ssem.at[g], msg_rsem.at[0, g], 2)
        for k in range(2):
            grow[g, k] = row8(ext_row_in[g, k])
            gcol[g, k] = ext_col_in[g, k]
        gb = gcol[g, 1]
        E[g, 0] = E[g, 0] - jnp.where(subw == 0, grow[g, 0], 0.0)
        for t in range(T):
            E[g, t, :, :LANES] = E[g, t, :, :LANES] - jnp.where(lane == 0, turn_lanes(gb, -t), 0.0)

    def slopes(slot, g):
        wait_halos(slot, g)
        u = row8(row_recv[slot, 1, g])
        u_right = to_left(u, row8(turn_lanes(corner_recv[slot, 0, g], LANES - 1)))
        zero = jnp.zeros_like(u)
        slope_row[g, 0] = jnp.where(up, row8(row_send[slot, 0, g]) - u, zero)
        slope_row[g, 1] = jnp.where(up, u_right - u, zero)
        u = col_recv[slot, 1, g]
        turn = turn_lanes(pltpu.roll(u, SUBS - 1, 0), T - 1)
        turn = jnp.where(sub == SUBS - 1, row8(turn_lanes(corner_recv[slot, 1, g], T)), turn)
        u_down = jnp.where(lane == T - 1, turn, turn_lanes(u, -1))
        zero = jnp.zeros_like(u)
        slope_col[g, 0] = jnp.where(left, u_down - u, zero)
        slope_col[g, 1] = jnp.where(left, col_send[slot, 0, g] - u, zero)
        GA[g, T - 1] = GA[g, T - 1] + jnp.where(subw == SUBS - 1, row8(row_recv[slot, 0, g]), 0.0)
        beside = col_recv[slot, 0, g]
        for t in range(T):
            entering = jnp.where(lane == LANES - 1, turn_lanes(beside, LANES - 1 - t), 0.0)
            GB[g, t, :, C - LANES:] = GB[g, t, :, C - LANES:] + entering

    def shrink(va, vb, c):
        f = jnp.maximum(1.0 - c * lax.rsqrt(va * va + vb * vb), 0.0)
        return f * va, f * vb

    def adapt(slot, g):
        tau, sigma = tau_ref[g], sig_ref[g]
        wait_message(slot, g)
        primal, dual = (jnp.broadcast_to(v, (SUBS, LANES)) for v in totals(slot, g))
        primal = tau * tau * primal + epsilon
        dual = sigma * sigma * dual + epsilon
        root = lax.rsqrt(primal) * (dual * lax.rsqrt(dual))
        s = lax.rsqrt(root)
        tau = tau * (root * s)
        sigma = sigma * s
        tau_ref[g] = tau
        sig_ref[g] = sigma
        return s, tau, sigma

    def sweep(g, other, scale, tau, closing):
        wscale, wtwice = wide(scale), wide(tau + tau)
        ghost_a, ghost_b = shrink(
            wscale * grow[g, 0] + slope_row[g, 0], wscale * grow[g, 1] + slope_row[g, 1], row8(cost_row_in[...])
        )
        side_a, side_b = shrink(
            scale * gcol[g, 0] + slope_col[g, 0], scale * gcol[g, 1] + slope_col[g, 1], cost_col_in[...]
        )
        grow[g, 0] = ghost_a
        grow[g, 1] = ghost_b
        gcol[g, 0] = side_a
        gcol[g, 1] = side_b
        acc_p = jnp.zeros((SUBS, C), f32)
        acc_d = jnp.zeros((SUBS, C), f32)

        def dual(t, a2, above, b2):
            nonlocal acc_d
            q2 = wtwice * divergence(t, a2, above, b2, side_b)
            w = q2 - E[g, t]
            W[g, t] = w
            if closing:
                w = 0.5 * q2 - IM[g, t]
            acc_d = acc_d + w * w

        for t in range(T):
            a, b = wscale * A[g, t], wscale * B[g, t]
            a2, b2 = shrink(a + GA[g, t], b + GB[g, t], CO[t])
            A[g, t] = a2
            B[g, t] = b2
            if not closing:
                da, db = a2 - a, b2 - b
                acc_p = acc_p + (da * da + db * db)
            if t:
                dual(t, a2, above, b2)
            else:
                a_first, b_first = a2, b2
            above = a2
        dual(0, a_first, above_first(above, ghost_a), b_first)
        send_message(other, g, fold(acc_p, acc_d))

    ends = sorted({0, K - 1})

    def chunk(k):
        return pl.ds(k * LANES, LANES)

    def depart(other, g, sigma):
        packs = [ones, ones]
        for t in range(T):
            for k in range(K) if t in (0, T - 1) else ends:
                u2 = U[g, t, :, chunk(k)] + sigma * W[g, t, :, chunk(k)]
                U[g, t, :, chunk(k)] = u2
                if k == 0:
                    packs[0] = pack_first(packs[0], u2, t)
                if k == K - 1:
                    packs[1] = pack_last(packs[1], u2, t)
                if t == 0:
                    row_send[other, 0, g, :, chunk(k)] = u2[0:1]
                if t == T - 1:
                    row_send[other, 1, g, :, chunk(k)] = u2[SUBS - 1:]
        for k in range(2):
            col_send[other, k, g] = packs[k]
        start_all(halos(other, g))

    def settle(g, c):
        sigma = sig_ref[g]
        first = prev = U[g, 0]
        for t in range(T):
            w = W[g, t]
            E[g, t] = 0.5 * (w + E[g, t]) + IM[g, t]
            if t in (0, T - 1):
                u2 = U[g, t]
            else:
                inner = [
                    U[g, t, :, chunk(k)] if k in ends else U[g, t, :, chunk(k)] + sigma * w[:, k * LANES:(k + 1) * LANES]
                    for k in range(K)
                ]
                for k in range(K):
                    if k not in ends:
                        U[g, t, :, chunk(k)] = inner[k]
                u2 = jnp.concatenate(inner, axis=1)
            GB[g, t] = to_left(u2, no_lane) - u2
            if t:
                GA[g, t - 1] = u2 - prev
            if t == T - 1:
                GA[g, t] = below_last(first) - u2
            prev = u2
        return c

    def opening(g, c):
        begin(g)
        slopes(0, g)
        step = jnp.full((SUBS, LANES), initial_step, f32)
        tau_ref[g] = step
        sig_ref[g] = step
        @pl.when(g == 0)
        def _():
            wait_edges(out_sem.at[1], out_sem.at[2], 1)

        sweep(g, 1, 1.0 / step, step, False)
        depart(1, g, step)
        return c

    lax.fori_loop(0, G, opening, 0)
    lax.fori_loop(0, G, settle, 0)
    slopes(1, 0)

    def turn(i, c):
        slot = lax.rem(i, 2)
        other = 1 - slot

        def one(g, c):
            s, tau, sigma = adapt(slot, g)
            sweep(g, other, s, tau, False)
            depart(other, g, sigma)

            @pl.when(g < G - 1)
            def _():
                slopes(slot, g + 1)

            return c

        lax.fori_loop(0, G, one, c)
        lax.fori_loop(0, G, settle, c)
        slopes(other, 0)
        return c

    lax.fori_loop(1, ITERS - 1, turn, 0)
    slot = (ITERS - 1) % 2

    def close(g, c):
        s, tau, _ = adapt(slot, g)
        sweep(g, 1 - slot, s, tau, True)

        @pl.when(g < G - 1)
        def _():
            slopes(slot, g + 1)

        return c

    def unload(g, c):
        wtau, wsigma = wide(tau_ref[g]), wide(sig_ref[g])
        for t in range(T):
            scatter(flow_in, wtau * A[g, t], 0, g, t)
            scatter(flow_in, wtau * B[g, t], 1, g, t)
            scatter(u_in, U[g, t] + wsigma * W[g, t], g, t)
        return c

    lax.fori_loop(0, G, close, 0)
    lax.fori_loop(0, G, unload, 0)
    results = [
        pltpu.make_async_copy(src.at[k], piece(dst, k), out_sem.at[i])
        for i, (src, dst) in enumerate(((flow_in, flow_hbm_out), (u_in, u_hbm_out)))
        for k in range(K)
    ]
    for copy in results:
        copy.start()
    cells = T * SUBS * C * n
    row = ones
    for g in range(G):
        wait_message(1 - slot, g)
        row = jnp.where(lane == g, totals(1 - slot, g)[1] / cells, row)
    res_row[...] = row
    give = pltpu.make_async_copy(res_row, res_out, out_sem.at[2])
    give.start()
    for i, whole in enumerate((flow_hbm_out, u_hbm_out)):
        pltpu.make_async_copy(whole, whole, out_sem.at[i]).wait()
    give.wait()


def finish(flow_in, u_in, res_in, flow_out, u_out, res_out, row, short, sems):
    pick = pltpu.make_async_copy(res_in, row, sems.at[0])
    pick.start()
    copies = [pltpu.make_async_copy(u_in, u_out, sems.at[1]), pltpu.make_async_copy(flow_in, flow_out, sems.at[2])]
    for copy in copies:
        copy.start()
    pick.wait()
    short[...] = row[0:1, 0:short.shape[1]]
    give = pltpu.make_async_copy(short, res_out, sems.at[0])
    give.start()
    for copy in copies:
        copy.wait()
    give.wait()


def local(ny, nx, imbalance, flow, potential, cost):
    pairs, rows, cols = imbalance.shape
    T = rows // SUBS
    n = ny * nx
    assert rows % SUBS == 0 and cols % LANES == 0 and 4 <= T < LANES and ny % 2 == 0 and nx > 1
    assert pairs <= LANES
    G = pairs
    f32 = jnp.float32
    block = (pairs, T, SUBS, cols)
    packed = (SUBS, LANES)
    K = cols // LANES
    hbm = pl.BlockSpec(memory_space=pltpu.HBM)
    flow_out, u_out, res = pl.pallas_call(
        functools.partial(kernel, ny, nx),
        out_shape=(
            jax.ShapeDtypeStruct(flow.shape, f32),
            jax.ShapeDtypeStruct(potential.shape, f32),
            jax.ShapeDtypeStruct(packed, f32),
        ),
        in_specs=[hbm] * 4,
        out_specs=(hbm, hbm, hbm),
        scratch_shapes=[
            pltpu.VMEM((K, pairs, rows, LANES), f32), pltpu.VMEM((K, 2, pairs, rows, LANES), f32),
            pltpu.VMEM((K, pairs, rows, LANES), f32), pltpu.VMEM((K, rows, LANES), f32),
        ] + [pltpu.VMEM(block, f32)] * 8 + [
            pltpu.VMEM(block[1:], f32),
            pltpu.VMEM((G,) + packed, f32), pltpu.VMEM((G,) + packed, f32),
            pltpu.VMEM((2, 2, G, 1, cols), f32), pltpu.VMEM((2, 2, G) + packed, f32),
            pltpu.VMEM((2, 2, G, 1, cols), f32), pltpu.VMEM((2, 2, G) + packed, f32),
            pltpu.VMEM((2, 2, G, 1, LANES), f32),
            pltpu.VMEM((2, G, 2, LANES), f32), pltpu.VMEM((2, G, n, 2, LANES), f32),
            pltpu.VMEM((G, 2, 1, cols), f32), pltpu.VMEM((G, 2) + packed, f32),
            pltpu.VMEM((G, 2, 1, cols), f32), pltpu.VMEM((G, 2) + packed, f32),
            pltpu.VMEM((1, cols), f32), pltpu.VMEM(packed, f32),
            pltpu.VMEM((1, cols), f32), pltpu.VMEM(packed, f32),
            pltpu.VMEM((G, 2, SUBS, cols), f32), pltpu.VMEM((G, 2) + packed, f32),
            pltpu.VMEM((G, 2, SUBS, cols), f32), pltpu.VMEM((G, 2) + packed, f32),
            pltpu.VMEM(packed, f32), pltpu.VMEM((2 * K + 2 * SUBS + 2, 1, LANES), f32),
            pltpu.SemaphoreType.DMA((G,)), pltpu.SemaphoreType.DMA((2, G)),
            pltpu.SemaphoreType.DMA((G,)), pltpu.SemaphoreType.DMA((2, G)),
            pltpu.SemaphoreType.DMA((3,)), pltpu.SemaphoreType.REGULAR,
        ],
        compiler_params=pltpu.CompilerParams(
            collective_id=0, has_side_effects=True, vmem_limit_bytes=48 * 1024 * 1024
        ),
    )(*(pltpu.with_memory_space_constraint(x, pltpu.HBM) for x in (imbalance, flow, potential, cost)))
    anywhere = pl.BlockSpec(memory_space=pl.ANY)
    flow_out, u_out, res = pl.pallas_call(
        finish,
        out_shape=(
            jax.ShapeDtypeStruct(flow.shape, f32),
            jax.ShapeDtypeStruct(potential.shape, f32),
            jax.ShapeDtypeStruct((1, pairs), f32),
        ),
        in_specs=[anywhere] * 3,
        out_specs=(hbm, hbm, hbm),
        scratch_shapes=[pltpu.VMEM(packed, f32), pltpu.VMEM((1, pairs), f32), pltpu.SemaphoreType.DMA((3,))],
    )(*(pltpu.with_memory_space_constraint(x, pltpu.VMEM) for x in (flow_out, u_out, res)))
    return flow_out, u_out, res.reshape(pairs)


def solution(mesh):
    placed = (P(None, "gy", "gx"), P(None, None, "gy", "gx"), P(None, "gy", "gx"), P("gy", "gx"))
    return jax.shard_map(
        functools.partial(local, mesh.shape["gy"], mesh.shape["gx"]),
        mesh=mesh,
        in_specs=placed,
        out_specs=(P(None, None, "gy", "gx"), P(None, "gy", "gx"), P()),
        check_vma=False,
    )
```

```python
import functools
import itertools

import jax
import jax.numpy as jnp
from jax import lax
from jax.experimental import pallas as pl
from jax.experimental.pallas import tpu as pltpu
from jax.sharding import PartitionSpec as P

ITERS = 12
LANES = 128
SUBS = 8

initial_step = 0.35
epsilon = 1e-06
MESH = pl.DeviceIdType.MESH


def kernel(
    ny, nx,
    imb_hbm, flow_hbm, u_hbm, cost_hbm,
    flow_hbm_out, u_hbm_out, res_out,
    imb_in, flow_in, u_in, cost_in,
    A, B, U, E, W, GA, GB, IM, CO,
    tau_ref, sig_ref,
    row_send, col_send, row_recv, col_recv, corner_recv, msg_send, msg_recv,
    ext_row, ext_col, ext_row_in, ext_col_in, cost_row, cost_col, cost_row_in, cost_col_in,
    grow, gcol, slope_row, slope_col,
    res_row, spare,
    halo_ssem, halo_rsem, msg_ssem, msg_rsem, out_sem, plane_sem,
):
    G, T, _, C = A.shape
    n = ny * nx
    rows = T * SUBS
    gy, gx = lax.axis_index("gy"), lax.axis_index("gx")
    me = gy * nx + gx
    up, down, left, right = gy > 0, gy < ny - 1, gx > 0, gx < nx - 1
    f32 = jnp.float32
    K = C // LANES

    def piece(ref, k):
        return ref.at[(slice(None),) * (len(ref.shape) - 1) + (pl.ds(k * LANES, LANES),)]

    def fetch_sem(i, g):
        return (out_sem.at[1], msg_ssem.at[g], halo_ssem.at[g], out_sem.at[0])[i]

    def start_fetch(i, g):
        for k in range(K):
            at = pl.ds(k * LANES, LANES)
            src, dst = (
                (cost_hbm.at[:, at], cost_in.at[k]), (u_hbm.at[g, :, at], u_in.at[k, g]),
                (flow_hbm.at[:, g, :, at], flow_in.at[k, :, g]), (imb_hbm.at[:, :, at], imb_in.at[k]),
            )[i]
            pltpu.make_async_copy(src, dst, fetch_sem(i, g)).start()

    def wait_fetch(i, g):
        whole = (cost_in, u_in.at[:, g], flow_in.at[:, :, g], imb_in)[i]
        pltpu.make_async_copy(whole, whole, fetch_sem(i, g)).wait()

    half = ny // 2
    low = gy < half
    xs = [lax.rem(gx + d, nx) for d in range(nx)]
    order = sorted(range(nx), key=lambda d: -min(d, nx - d))
    high = jnp.where(low, ny - 1 - gy, gy) - half
    across = [half + lax.rem(high + half - j, half) for j in range(half)]
    places = [(jnp.where(low, y, ny - 1 - y), xs[d]) for y in across for d in order]
    for k in range(1, ny - half):
        y = half + lax.rem(high + k, ny - half)
        places += [(jnp.where(low, ny - 1 - y, y), xs[d]) for d in order]
    places += [(gy, xs[d]) for d in order if d]

    start_fetch(1, 0)
    start_fetch(2, 0)
    start_fetch(0, 0)
    barrier = pltpu.get_barrier_semaphore()

    def greet(where):
        pl.semaphore_signal(barrier, inc=1, device_id=where, device_id_type=MESH)

    odd = lax.rem(gy, 2)
    column = [(lax.rem(gy + 2 * k, ny), gx) for k in range(1, half)]
    mates = [(gy, xs[d]) for d in order if d] + [(gy + 1 - 2 * odd, xs[d]) for d in order]
    low_side, high_side = odd == 1, odd == 0
    outside = [
        (jnp.logical_and(low_side, down), (gy + 1, gx)),
        (jnp.logical_and(low_side, jnp.logical_and(down, left)), (gy + 1, gx - 1)),
        (jnp.logical_and(high_side, up), (gy - 1, gx)),
        (jnp.logical_and(high_side, jnp.logical_and(up, right)), (gy - 1, gx + 1)),
    ]
    for where in column + mates:
        greet(where)
    guests = len(column) + len(mates)
    for ok, where in outside:
        guests = guests + jnp.where(ok, 1, 0)

        @pl.when(ok)
        def _(where=where):
            greet(where)

    def later(g, c):
        start_fetch(1, g)
        start_fetch(2, g)
        return c

    lax.fori_loop(1, G, later, 0)

    start_fetch(3, 0)

    def gather(ref, *index):
        at = pl.ds(index[-1], SUBS, stride=T)
        return jnp.concatenate([ref[(k,) + index[:-1] + (at, slice(None))] for k in range(K)], axis=1)

    def scatter(ref, value, *index):
        at = pl.ds(index[-1], SUBS, stride=T)
        for k in range(K):
            ref[(k,) + index[:-1] + (at, slice(None))] = value[:, k * LANES:(k + 1) * LANES]

    def line(ref, *index):
        return jnp.concatenate([ref[(k,) + index[:-1] + (pl.ds(index[-1], 1), slice(None))] for k in range(K)], axis=1)

    lane = lax.broadcasted_iota(jnp.int32, (SUBS, LANES), 1)
    sub = lax.broadcasted_iota(jnp.int32, (SUBS, LANES), 0)
    subw = lax.broadcasted_iota(jnp.int32, (SUBS, C), 0)
    ones = jnp.ones((SUBS, LANES), f32)

    def wide(x):
        return jnp.concatenate([x] * K, axis=1)

    def row8(x):
        return jnp.broadcast_to(x, (SUBS, x.shape[1]))

    def turn_lanes(x, by):
        return pltpu.roll(x, by % LANES, 1) if by % LANES else x

    def to_left(x, entering):
        r = [pltpu.roll(x[:, k * LANES:(k + 1) * LANES], LANES - 1, 1) for k in range(K)] + [entering]
        return jnp.concatenate([jnp.where(lane == LANES - 1, r[k + 1], r[k]) for k in range(K)], axis=1)

    def to_right(x, entering):
        r = [entering] + [pltpu.roll(x[:, k * LANES:(k + 1) * LANES], 1, 1) for k in range(K)]
        return jnp.concatenate([jnp.where(lane == 0, r[k], r[k + 1]) for k in range(K)], axis=1)

    def pack_first(acc, v, t):
        return jnp.where(lane == t, turn_lanes(v, t), acc)

    def pack_last(acc, v, t):
        return jnp.where(lane == t, turn_lanes(v, t + 1), acc)

    def remote(src, dst, ssem, rsem, where):
        return pltpu.make_async_remote_copy(
            src_ref=src, dst_ref=dst, send_sem=ssem, recv_sem=rsem, device_id=where, device_id_type=MESH
        )

    def halos(slot, g):
        sems = (halo_ssem.at[g], halo_rsem.at[slot, g])
        head, tail = row_send.at[slot, 0, g], row_send.at[slot, 1, g]
        return [
            (jnp.logical_and(down, left), remote(tail.at[:, pl.ds(0, LANES)], corner_recv.at[slot, 0, g], *sems, (gy + 1, gx - 1))),
            (jnp.logical_and(up, right), remote(head.at[:, pl.ds(C - LANES, LANES)], corner_recv.at[slot, 1, g], *sems, (gy - 1, gx + 1))),
            (up, remote(head, row_recv.at[slot, 0, g], *sems, (gy - 1, gx))),
            (down, remote(tail, row_recv.at[slot, 1, g], *sems, (gy + 1, gx))),
            (left, remote(col_send.at[slot, 0, g], col_recv.at[slot, 0, g], *sems, (gy, gx - 1))),
            (right, remote(col_send.at[slot, 1, g], col_recv.at[slot, 1, g], *sems, (gy, gx + 1))),
        ]

    def extras(g):
        sems = (msg_ssem.at[g], msg_rsem.at[0, g])
        return [
            (down, remote(ext_row.at[g], ext_row_in.at[g], *sems, (gy + 1, gx))),
            (right, remote(ext_col.at[g], ext_col_in.at[g], *sems, (gy, gx + 1))),
        ]

    def prices():
        sems = (out_sem.at[1], out_sem.at[2])
        return [
            (down, remote(cost_row, cost_row_in, *sems, (gy + 1, gx))),
            (right, remote(cost_col, cost_col_in, *sems, (gy, gx + 1))),
        ]

    def start_all(copies):
        for ok, copy in copies:
            @pl.when(ok)
            def _(copy=copy):
                copy.start()

    sides = [c for c in itertools.product((0, 1), repeat=4) if (c[0] or c[1]) and (c[2] or c[3])]

    def lies(case):
        flags = [f if has else jnp.logical_not(f) for f, has in zip((up, down, left, right), case)]
        return functools.reduce(jnp.logical_and, flags)

    def wait_rows(sem, count):
        totals_of = {}
        for case in sides:
            totals_of.setdefault(count(*case), []).append(case)
        for total, cases in totals_of.items():
            if total:
                @pl.when(functools.reduce(jnp.logical_or, [lies(case) for case in cases]))
                def _(total=total):
                    whole = spare.at[pl.ds(0, total)]
                    pltpu.make_async_copy(whole, whole, sem).wait()

    def wait_halos(sem):
        wait_rows(sem, lambda u, d, l, r: K * (u + d) + SUBS * (l + r) + u * r + d * l)

    def halos_sent(g, c):
        wait_halos(halo_ssem.at[g])
        return c

    def wait_edges(ssem, rsem, parts):
        wait_rows(rsem, lambda u, d, l, r: parts * (K * u + SUBS * l))
        wait_rows(ssem, lambda u, d, l, r: parts * (K * d + SUBS * r))

    def send_message(slot, g, rows):
        for k, row in enumerate(rows):
            msg_send[slot, g, k:k + 1] = row
            msg_recv[slot, g, me, k:k + 1] = row
        for where in places:
            remote(
                msg_send.at[slot, g], msg_recv.at[slot, g, me], msg_ssem.at[g], msg_rsem.at[slot, g], where
            ).start()

    def wait_message(slot, g):
        whole = msg_recv.at[slot, g, pl.ds(0, n - 1)]
        pltpu.make_async_copy(whole, whole, msg_rsem.at[slot, g]).wait()

    def message_sent(g):
        whole = msg_recv.at[0, g, pl.ds(0, n - 1)]
        pltpu.make_async_copy(whole, whole, msg_ssem.at[g]).wait()

    def totals(slot, g):
        parts = [msg_recv[slot, g, k] for k in range(n)]
        while len(parts) > 1:
            parts = [sum(parts[k + 1:k + 2], parts[k]) for k in range(0, len(parts), 2)]
        return [jnp.sum(row8(parts[0][k:k + 1]), axis=1, keepdims=True) for k in range(2)]

    def fold(x, y):
        x, y = (sum((v[:, k * LANES:(k + 1) * LANES] for k in range(1, K)), v[:, :LANES]) for v in (x, y))
        half = SUBS // 2
        z = jnp.where(sub < half, x + pltpu.roll(x, half, 0), y + pltpu.roll(y, half, 0))
        z = z + pltpu.roll(z, 1, 0)
        z = z + pltpu.roll(z, 2, 0)
        return z[half - 1:half], z[SUBS - 1:]


    def edges(g, c):
        wait_fetch(1, g)
        packs = [ones] * 4
        row_send[0, 0, g] = line(u_in, g, 0)
        row_send[0, 1, g] = line(u_in, g, rows - 1)
        for t in range(T):
            at = pl.ds(t, SUBS, stride=T)
            packs[0] = pack_first(packs[0], u_in[0, g, at, :], t)
            packs[1] = pack_last(packs[1], u_in[K - 1, g, at, :], t)
        wait_fetch(2, g)
        for t in range(T):
            at = pl.ds(t, SUBS, stride=T)
            packs[2] = pack_last(packs[2], flow_in[K - 1, 0, g, at, :], t)
            packs[3] = pack_last(packs[3], flow_in[K - 1, 1, g, at, :], t)
        col_send[0, 0, g] = packs[0]
        col_send[0, 1, g] = packs[1]
        for k in range(2):
            ext_col[g, k] = packs[2 + k]
            ext_row[g, k] = line(flow_in, k, g, rows - 1)
        return c

    for missing, refs in (
        (jnp.logical_not(down), [row_recv.at[s, 0] for s in range(2)]),
        (jnp.logical_not(up), [row_recv.at[s, 1] for s in range(2)] + [ext_row_in]),
        (jnp.logical_not(right), [col_recv.at[s, 0] for s in range(2)]),
        (jnp.logical_not(left), [col_recv.at[s, 1] for s in range(2)] + [ext_col_in]),
        (jnp.logical_not(jnp.logical_and(up, right)), [corner_recv.at[s, 0] for s in range(2)]),
        (jnp.logical_not(jnp.logical_and(down, left)), [corner_recv.at[s, 1] for s in range(2)]),
    ):
        @pl.when(missing)
        def _(refs=refs):
            for ref in refs:
                ref[...] = jnp.zeros(ref.shape, f32)

    for missing, ref in ((jnp.logical_not(up), cost_row_in), (jnp.logical_not(left), cost_col_in)):
        @pl.when(missing)
        def _(ref=ref):
            ref[...] = jnp.ones(ref.shape, f32)

    edges(0, 0)
    pl.semaphore_wait(barrier, guests)
    for where in column:
        pl.semaphore_signal(plane_sem, inc=1, device_id=where, device_id_type=MESH)
    start_all(halos(0, 0) + extras(0))
    wait_fetch(0, 0)
    pack = ones
    for t in range(T):
        CO[t] = gather(cost_in, t)
        pack = pack_last(pack, CO[t][:, C - LANES:], t)
    cost_col[...] = pack
    cost_row[...] = line(cost_in, rows - 1)
    start_all(prices())

    def announce(g, c):
        edges(g, c)
        start_all(halos(0, g) + extras(g))
        return c

    lax.fori_loop(1, G, announce, 0)

    no_lane = jnp.zeros((SUBS, LANES), f32)

    def above_first(a_last, ghost):
        return jnp.where(subw == 0, ghost, pltpu.roll(a_last, 1, 0))

    def below_last(u_first):
        return jnp.where(subw == SUBS - 1, 0.0, pltpu.roll(u_first, SUBS - 1, 0))

    wait_fetch(3, 0)

    def load(g, c):
        for t in range(T):
            A[g, t] = gather(flow_in, 0, g, t)
            B[g, t] = gather(flow_in, 1, g, t)
            U[g, t] = gather(u_in, g, t)
            IM[g, t] = gather(imb_in, g, t)
        for t in range(T):
            a, b, u = A[g, t], B[g, t], U[g, t]
            above = A[g, t - 1] if t else above_first(A[g, T - 1], 0.0)
            E[g, t] = ((a - above) + (b - to_right(b, no_lane))) + IM[g, t]
            GA[g, t] = (U[g, t + 1] if t < T - 1 else below_last(U[g, 0])) - u
            GB[g, t] = to_left(u, no_lane) - u
        return c

    lax.fori_loop(0, G, load, 0)
    pl.semaphore_wait(plane_sem, len(column))

    def divergence(t, a, above, b, gb):
        return ((a - above) + (b - to_right(b, turn_lanes(gb, -t))))

    def begin(g):
        wait_edges(msg_ssem.at[g], msg_rsem.at[0, g], 2)
        halos_sent(g, 0)
        for k in range(2):
            grow[g, k] = row8(ext_row_in[g, k])
            gcol[g, k] = ext_col_in[g, k]
        gb = gcol[g, 1]
        E[g, 0] = E[g, 0] - jnp.where(subw == 0, grow[g, 0], 0.0)
        for t in range(T):
            E[g, t, :, :LANES] = E[g, t, :, :LANES] - jnp.where(lane == 0, turn_lanes(gb, -t), 0.0)

    def slopes(slot, g):
        wait_halos(halo_rsem.at[slot, g])
        u = row8(row_recv[slot, 1, g])
        u_right = to_left(u, row8(turn_lanes(corner_recv[slot, 0, g], LANES - 1)))
        zero = jnp.zeros_like(u)
        slope_row[g, 0] = jnp.where(up, row8(row_send[slot, 0, g]) - u, zero)
        slope_row[g, 1] = jnp.where(up, u_right - u, zero)
        u = col_recv[slot, 1, g]
        turn = turn_lanes(pltpu.roll(u, SUBS - 1, 0), T - 1)
        turn = jnp.where(sub == SUBS - 1, row8(turn_lanes(corner_recv[slot, 1, g], T)), turn)
        u_down = jnp.where(lane == T - 1, turn, turn_lanes(u, -1))
        zero = jnp.zeros_like(u)
        slope_col[g, 0] = jnp.where(left, u_down - u, zero)
        slope_col[g, 1] = jnp.where(left, col_send[slot, 0, g] - u, zero)
        GA[g, T - 1] = GA[g, T - 1] + jnp.where(subw == SUBS - 1, row8(row_recv[slot, 0, g]), 0.0)
        beside = col_recv[slot, 0, g]
        for t in range(T):
            entering = jnp.where(lane == LANES - 1, turn_lanes(beside, LANES - 1 - t), 0.0)
            GB[g, t, :, C - LANES:] = GB[g, t, :, C - LANES:] + entering

    def shrink(va, vb, c):
        f = jnp.maximum(1.0 - c * lax.rsqrt(va * va + vb * vb), 0.0)
        return f * va, f * vb

    def adapt(slot, g):
        tau, sigma = tau_ref[g], sig_ref[g]
        wait_message(slot, g)
        primal, dual = (jnp.broadcast_to(v, (SUBS, LANES)) for v in totals(slot, g))
        primal = tau * tau * primal + epsilon
        dual = sigma * sigma * dual + epsilon
        root = lax.rsqrt(primal) * (dual * lax.rsqrt(dual))
        s = lax.rsqrt(root)
        tau = tau * (root * s)
        sigma = sigma * s
        tau_ref[g] = tau
        sig_ref[g] = sigma
        return s, tau, sigma

    def sweep(g, other, scale, tau, closing):
        wscale, wtwice = wide(scale), wide(tau + tau)
        ghost_a, ghost_b = shrink(
            wscale * grow[g, 0] + slope_row[g, 0], wscale * grow[g, 1] + slope_row[g, 1], row8(cost_row_in[...])
        )
        side_a, side_b = shrink(
            scale * gcol[g, 0] + slope_col[g, 0], scale * gcol[g, 1] + slope_col[g, 1], cost_col_in[...]
        )
        grow[g, 0] = ghost_a
        grow[g, 1] = ghost_b
        gcol[g, 0] = side_a
        gcol[g, 1] = side_b
        acc_p = jnp.zeros((SUBS, C), f32)
        acc_d = jnp.zeros((SUBS, C), f32)

        def dual(t, a2, above, b2):
            nonlocal acc_d
            q2 = wtwice * divergence(t, a2, above, b2, side_b)
            w = q2 - E[g, t]
            W[g, t] = w
            if closing:
                w = 0.5 * q2 - IM[g, t]
            acc_d = acc_d + w * w

        for t in range(T):
            a, b = wscale * A[g, t], wscale * B[g, t]
            a2, b2 = shrink(a + GA[g, t], b + GB[g, t], CO[t])
            A[g, t] = a2
            B[g, t] = b2
            if not closing:
                da, db = a2 - a, b2 - b
                acc_p = acc_p + (da * da + db * db)
            if t:
                dual(t, a2, above, b2)
            else:
                a_first, b_first = a2, b2
            above = a2
        dual(0, a_first, above_first(above, ghost_a), b_first)
        send_message(other, g, fold(acc_p, acc_d))

    ends = sorted({0, K - 1})

    def chunk(k):
        return pl.ds(k * LANES, LANES)

    def depart(other, g, sigma):
        packs = [ones, ones]
        for t in range(T):
            for k in range(K) if t in (0, T - 1) else ends:
                u2 = U[g, t, :, chunk(k)] + sigma * W[g, t, :, chunk(k)]
                U[g, t, :, chunk(k)] = u2
                if k == 0:
                    packs[0] = pack_first(packs[0], u2, t)
                if k == K - 1:
                    packs[1] = pack_last(packs[1], u2, t)
                if t == 0:
                    row_send[other, 0, g, :, chunk(k)] = u2[0:1]
                if t == T - 1:
                    row_send[other, 1, g, :, chunk(k)] = u2[SUBS - 1:]
        for k in range(2):
            col_send[other, k, g] = packs[k]
        start_all(halos(other, g))

    def settle(g, c):
        message_sent(g)
        sigma = sig_ref[g]
        first = prev = U[g, 0]
        for t in range(T):
            w = W[g, t]
            E[g, t] = 0.5 * (w + E[g, t]) + IM[g, t]
            if t in (0, T - 1):
                u2 = U[g, t]
            else:
                inner = [
                    U[g, t, :, chunk(k)] if k in ends else U[g, t, :, chunk(k)] + sigma * w[:, k * LANES:(k + 1) * LANES]
                    for k in range(K)
                ]
                for k in range(K):
                    if k not in ends:
                        U[g, t, :, chunk(k)] = inner[k]
                u2 = jnp.concatenate(inner, axis=1)
            GB[g, t] = to_left(u2, no_lane) - u2
            if t:
                GA[g, t - 1] = u2 - prev
            if t == T - 1:
                GA[g, t] = below_last(first) - u2
            prev = u2
        return c

    def opening(g, c):
        begin(g)
        slopes(0, g)
        step = jnp.full((SUBS, LANES), initial_step, f32)
        tau_ref[g] = step
        sig_ref[g] = step
        @pl.when(g == 0)
        def _():
            wait_edges(out_sem.at[1], out_sem.at[2], 1)

        sweep(g, 1, 1.0 / step, step, False)
        depart(1, g, step)
        return c

    lax.fori_loop(0, G, opening, 0)
    lax.fori_loop(0, G, settle, 0)
    lax.fori_loop(0, G, halos_sent, 0)
    slopes(1, 0)

    def turn(i, c):
        slot = lax.rem(i, 2)
        other = 1 - slot

        def one(g, c):
            s, tau, sigma = adapt(slot, g)
            sweep(g, other, s, tau, False)
            depart(other, g, sigma)

            @pl.when(g < G - 1)
            def _():
                slopes(slot, g + 1)

            return c

        lax.fori_loop(0, G, one, c)
        lax.fori_loop(0, G, settle, c)
        lax.fori_loop(0, G, halos_sent, c)
        slopes(other, 0)
        return c

    lax.fori_loop(1, ITERS - 1, turn, 0)
    slot = (ITERS - 1) % 2

    def close(g, c):
        s, tau, _ = adapt(slot, g)
        sweep(g, 1 - slot, s, tau, True)

        @pl.when(g < G - 1)
        def _():
            slopes(slot, g + 1)

        return c

    def unload(g, c):
        wtau, wsigma = wide(tau_ref[g]), wide(sig_ref[g])
        for t in range(T):
            scatter(flow_in, wtau * A[g, t], 0, g, t)
            scatter(flow_in, wtau * B[g, t], 1, g, t)
            scatter(u_in, U[g, t] + wsigma * W[g, t], g, t)
        return c

    lax.fori_loop(0, G, close, 0)
    lax.fori_loop(0, G, unload, 0)
    results = [
        pltpu.make_async_copy(src.at[k], piece(dst, k), out_sem.at[i])
        for i, (src, dst) in enumerate(((flow_in, flow_hbm_out), (u_in, u_hbm_out)))
        for k in range(K)
    ]
    for copy in results:
        copy.start()
    cells = T * SUBS * C * n
    row = ones
    for g in range(G):
        message_sent(g)
        wait_message(1 - slot, g)
        row = jnp.where(lane == g, totals(1 - slot, g)[1] / cells, row)
    res_row[...] = row
    give = pltpu.make_async_copy(res_row, res_out, out_sem.at[2])
    give.start()
    for i, whole in enumerate((flow_hbm_out, u_hbm_out)):
        pltpu.make_async_copy(whole, whole, out_sem.at[i]).wait()
    give.wait()


def finish(flow_in, u_in, res_in, flow_out, u_out, res_out, row, short, sems):
    pick = pltpu.make_async_copy(res_in, row, sems.at[0])
    pick.start()
    copies = [pltpu.make_async_copy(u_in, u_out, sems.at[1]), pltpu.make_async_copy(flow_in, flow_out, sems.at[2])]
    for copy in copies:
        copy.start()
    pick.wait()
    short[...] = row[0:1, 0:short.shape[1]]
    give = pltpu.make_async_copy(short, res_out, sems.at[0])
    give.start()
    for copy in copies:
        copy.wait()
    give.wait()


def local(ny, nx, imbalance, flow, potential, cost):
    pairs, rows, cols = imbalance.shape
    T = rows // SUBS
    n = ny * nx
    assert rows % SUBS == 0 and cols % LANES == 0 and 4 <= T < LANES and ny % 2 == 0 and nx > 1
    assert pairs <= LANES
    G = pairs
    f32 = jnp.float32
    block = (pairs, T, SUBS, cols)
    packed = (SUBS, LANES)
    K = cols // LANES
    hbm = pl.BlockSpec(memory_space=pltpu.HBM)
    flow_out, u_out, res = pl.pallas_call(
        functools.partial(kernel, ny, nx),
        out_shape=(
            jax.ShapeDtypeStruct(flow.shape, f32),
            jax.ShapeDtypeStruct(potential.shape, f32),
            jax.ShapeDtypeStruct(packed, f32),
        ),
        in_specs=[hbm] * 4,
        out_specs=(hbm, hbm, hbm),
        scratch_shapes=[
            pltpu.VMEM((K, pairs, rows, LANES), f32), pltpu.VMEM((K, 2, pairs, rows, LANES), f32),
            pltpu.VMEM((K, pairs, rows, LANES), f32), pltpu.VMEM((K, rows, LANES), f32),
        ] + [pltpu.VMEM(block, f32)] * 8 + [
            pltpu.VMEM(block[1:], f32),
            pltpu.VMEM((G,) + packed, f32), pltpu.VMEM((G,) + packed, f32),
            pltpu.VMEM((2, 2, G, 1, cols), f32), pltpu.VMEM((2, 2, G) + packed, f32),
            pltpu.VMEM((2, 2, G, 1, cols), f32), pltpu.VMEM((2, 2, G) + packed, f32),
            pltpu.VMEM((2, 2, G, 1, LANES), f32),
            pltpu.VMEM((2, G, 2, LANES), f32), pltpu.VMEM((2, G, n, 2, LANES), f32),
            pltpu.VMEM((G, 2, 1, cols), f32), pltpu.VMEM((G, 2) + packed, f32),
            pltpu.VMEM((G, 2, 1, cols), f32), pltpu.VMEM((G, 2) + packed, f32),
            pltpu.VMEM((1, cols), f32), pltpu.VMEM(packed, f32),
            pltpu.VMEM((1, cols), f32), pltpu.VMEM(packed, f32),
            pltpu.VMEM((G, 2, SUBS, cols), f32), pltpu.VMEM((G, 2) + packed, f32),
            pltpu.VMEM((G, 2, SUBS, cols), f32), pltpu.VMEM((G, 2) + packed, f32),
            pltpu.VMEM(packed, f32), pltpu.VMEM((2 * K + 2 * SUBS + 2, 1, LANES), f32),
            pltpu.SemaphoreType.DMA((G,)), pltpu.SemaphoreType.DMA((2, G)),
            pltpu.SemaphoreType.DMA((G,)), pltpu.SemaphoreType.DMA((2, G)),
            pltpu.SemaphoreType.DMA((3,)), pltpu.SemaphoreType.REGULAR,
        ],
        compiler_params=pltpu.CompilerParams(
            collective_id=0, has_side_effects=True, vmem_limit_bytes=48 * 1024 * 1024
        ),
    )(*(pltpu.with_memory_space_constraint(x, pltpu.HBM) for x in (imbalance, flow, potential, cost)))
    anywhere = pl.BlockSpec(memory_space=pl.ANY)
    flow_out, u_out, res = pl.pallas_call(
        finish,
        out_shape=(
            jax.ShapeDtypeStruct(flow.shape, f32),
            jax.ShapeDtypeStruct(potential.shape, f32),
            jax.ShapeDtypeStruct((1, pairs), f32),
        ),
        in_specs=[anywhere] * 3,
        out_specs=(hbm, hbm, hbm),
        scratch_shapes=[pltpu.VMEM(packed, f32), pltpu.VMEM((1, pairs), f32), pltpu.SemaphoreType.DMA((3,))],
    )(*(pltpu.with_memory_space_constraint(x, pltpu.VMEM) for x in (flow_out, u_out, res)))
    return flow_out, u_out, res.reshape(pairs)


def solution(mesh):
    placed = (P(None, "gy", "gx"), P(None, None, "gy", "gx"), P(None, "gy", "gx"), P("gy", "gx"))
    return jax.shard_map(
        functools.partial(local, mesh.shape["gy"], mesh.shape["gx"]),
        mesh=mesh,
        in_specs=placed,
        out_specs=(P(None, None, "gy", "gx"), P(None, "gy", "gx"), P()),
        check_vma=False,
    )
```
